32 devices in a mesh: group: 2 (over x), row: 4 (over y, core), col: 4 (over z).
Axes of the slice: x: 2, y: 2, z: 4, core: 2. Of those that a mesh axis runs over, the one named last changes fastest.
Arguments:
- pair_repr: bfloat16 [128, 128, 128], P(('group', 'row'), 'col'), may hold values from -6 to 6
- pair_mask: int32 [128, 128], P(('group', 'row'), 'col'), may hold values 0 or 1
- chain_id: int32 [128], replicated, may hold values from 0 to 7, never falling along the last dimension, each value on 1 to 32 neighbouring positions
- tri_in_gain: float32 [128], replicated, may hold values from 0.5 to 1.5
- tri_proj: bfloat16 [128, 512], replicated, may hold values from -0.5 to 0.5
- tri_gate: bfloat16 [128, 128], replicated, may hold values from -0.5 to 0.5
- tri_out_gain: float32 [128], replicated, may hold values from 0.5 to 1.5
- tri_out: bfloat16 [128, 128], replicated, may hold values from -0.5 to 0.5
- bias_gain: float32 [128], replicated, may hold values from 0.5 to 1.5
- bias_weight: bfloat16 [128, 16], replicated, may hold values from -0.5 to 0.5
- chain_bias: float32 [16], replicated, may hold values from -2 to 2
- tokens: bfloat16 [24, 128, 768], P(('group', 'row')), may hold values from -6 to 6
- noise_level: int32 [24], P(('group', 'row')), may hold values from 0 to 199
- attn_gain: float32 [768], replicated, may hold values from 0.5 to 1.5
- attn_weight: bfloat16 [4, 768, 768], P(None, None, 'col'), may hold values from -0.21875 to 0.21875
- out_weight: bfloat16 [768, 768], P('col'), may hold values from -0.21875 to 0.21875
- cotangent: bfloat16 [24, 128, 768], P(('group', 'row')), may hold values from -6 to 6
Outputs:
- pair_next: bfloat16 [128, 128, 128], P(('group', 'row'), 'col')
- pair_grad: float32 [128, 128, 128], P(('group', 'row'), 'col')
- bias_weight_grad: float32 [128, 16], replicated
- denoised: bfloat16 [24, 128, 768], P(('group', 'row'), 'col')
- token_grad: bfloat16 [24, 128, 768], P(('group', 'row'), 'col')
- attn_weight_grad: float32 [4, 768, 768], P(None, ('group', 'row'), 'col')
- out_weight_grad: float32 [768, 768], P('col', ('group', 'row'))
The draws below stay inside these ranges and needn't reach their ends.
Inputs may be any that keep to these rules, and one draw needn't show every extreme that they name: `chain_id`: chain numbers never fall along the tokens.
All inputs are finite; a program needn't handle non-finite values. No bound on the sum of `pair_mask` on one device may be relied on, other than what follows from the above.
Results may differ from the reference program's by a relative error of at most 0.014.
Values may be sent and summed in bfloat16 or wider, within the bound.
No kernel may reach another device: no remote copies, remote signals or barrier semaphores. Data moves between devices by JAX's collectives and lax.ppermute only.
A program may use at most 64 MiB of HBM per device.

```python
import math
import jax
import jax.numpy as jnp
import numpy as np
from jax import lax

C = 128
H = 16
D = 768
LEVELS = 200
CHAINS = 8
N = 128
COPIES = 24


def touch_ends(result, rng, least, largest):
    place = [jax.random.randint(jax.random.fold_in(rng, axis), (), 0, length) for axis, length in enumerate(result.shape)]
    longest = result.shape.index(max(result.shape))
    neighbour = place[:longest] + [(place[longest] + 1) % result.shape[longest]] + place[longest + 1:]
    return result.at[tuple(place)].set(least).at[tuple(neighbour)].set(largest)


def shard_levels(rng, dims, split, least, high):
    factor_of, own = 1.0, jax.random.fold_in(rng, 6)
    for dim, blocks in split:
        steps = jnp.exp(jax.random.uniform(jax.random.fold_in(own, dim), (blocks,), jnp.float32, least / len(split), high / len(split)))
        factor_of = factor_of * jnp.repeat(steps, dims[dim] // blocks).reshape([-1 if axis == dim else 1 for axis in range(len(dims))])
    return factor_of


def split_up(number_of, total, reach, lean):
    loads = [(1 << 20) // math.isqrt(standing ** lean) + 1 for standing in range(2, number_of + 1)]
    spare, counts = total - reach - (number_of - 1), [1] * (number_of - 1)
    while spare > 0:
        candidates = [i for i in range(number_of - 1) if counts[i] < reach]
        pool, left = sum([loads[i] for i in candidates]), spare
        for i in candidates:
            more = min(reach - counts[i], max(1, left * loads[i] // pool), spare)
            counts[i] = counts[i] + more
            spare = spare - more
    return np.array([reach] + counts)


def ragged_sizes(key, amount, total, reach, lean):
    if amount == 2:
        one = jax.random.randint(key, (), max(1, total - reach), min(reach, total - 1) + 1)
        return jnp.stack([one, total - one])
    lengths = jnp.asarray(split_up(amount, total, reach, lean), jnp.int32)
    pairs = (amount - 1) // 2
    giver, sink = lengths[1:1 + 2 * pairs:2], lengths[2:2 + 2 * pairs:2]
    margin = jnp.minimum(giver - 1, reach - sink)
    passed = jax.random.randint(jax.random.fold_in(key, 1), (pairs,), 0, 1 << 20) % (margin + 1)
    lengths = lengths.at[1:1 + 2 * pairs:2].set(giver - passed).at[2:2 + 2 * pairs:2].set(sink + passed)
    return lengths[jax.random.permutation(jax.random.fold_in(key, 2), amount)]


def normal_values(rng, dims, width, most, shards=(), kind=jnp.bfloat16):
    gain = shard_levels(rng, dims, shards, -0.22, 0.18) if shards else 1.0
    entries = jax.random.normal(rng, dims, jnp.float32) * width * gain
    return jnp.minimum(jnp.maximum(entries, -most), most).astype(kind)


def setup_inputs(seed: int = 0) -> dict:
    arg_keys = jax.random.split(jax.random.key(seed), 18)
    return {
        "pair_repr": normal_values(arg_keys[0], (N, N, C), 1.0, 6.0, ((0, 8), (1, 4))),
        "pair_mask": touch_ends((jax.random.randint(arg_keys[1], (N, N), 0, 4) < 3).astype(jnp.int32), jax.random.fold_in(arg_keys[1], 1), 0, 1),
        "chain_id": jnp.searchsorted(jnp.cumsum(ragged_sizes(arg_keys[2], CHAINS, N, N // 4, 1)), jnp.arange(N), side="right").astype(jnp.int32),
        "tri_in_gain": jnp.clip(1.0 + 0.1 * jax.random.normal(arg_keys[3], (C,), jnp.float32), 0.5, 1.5),
        "tri_proj": normal_values(arg_keys[4], (C, 4 * C), C ** -0.5, 0.5),
        "tri_gate": normal_values(arg_keys[5], (C, C), C ** -0.5, 0.5),
        "tri_out_gain": jnp.clip(1.0 + 0.1 * jax.random.normal(arg_keys[6], (C,), jnp.float32), 0.5, 1.5),
        "tri_out": normal_values(arg_keys[7], (C, C), C ** -0.5, 0.5),
        "bias_gain": jnp.clip(1.0 + 0.1 * jax.random.normal(arg_keys[8], (C,), jnp.float32), 0.5, 1.5),
        "bias_weight": normal_values(arg_keys[9], (C, H), C ** -0.5, 0.5),
        "chain_bias": jnp.clip(jax.random.uniform(arg_keys[10], (H,), jnp.float32, -2.0, 2.0), -2.0, 2.0),
        "tokens": normal_values(arg_keys[11], (COPIES, N, D), 1.0, 6.0, ((0, 8),)),
        "noise_level": touch_ends(jax.random.randint(arg_keys[12], (COPIES,), 0, LEVELS), jax.random.fold_in(arg_keys[12], 1), 0, LEVELS - 1).astype(jnp.int32),
        "attn_gain": jnp.clip(1.0 + 0.1 * jax.random.normal(arg_keys[13], (D,), jnp.float32), 0.5, 1.5),
        "attn_weight": normal_values(arg_keys[14], (4, D, D), D ** -0.5, 0.21875, ((2, 4),)),
        "out_weight": normal_values(arg_keys[15], (D, D), D ** -0.5, 0.21875, ((0, 4),)),
        "cotangent": normal_values(arg_keys[16], (COPIES, N, D), 1.0, 6.0, ((0, 8),)),
    }


EPSILON = 1e-05
SIGMA_LOW = 0.1
SIGMA_SPAN = 100.0

def normalize(values):
    average = lax.optimization_barrier(jnp.mean(values, -1, keepdims=True))
    centred = values - average
    return centred * lax.rsqrt(lax.optimization_barrier(jnp.mean(centred * centred, -1, keepdims=True)) + EPSILON)

def norm_back(gradient, values, norm_gain):
    average = lax.optimization_barrier(jnp.mean(values, -1, keepdims=True))
    centred = values - average
    inverse = lax.rsqrt(lax.optimization_barrier(jnp.mean(centred * centred, -1, keepdims=True)) + EPSILON)
    normed = centred * inverse
    weighted = gradient * norm_gain
    return inverse * (weighted - lax.optimization_barrier(jnp.mean(weighted, -1, keepdims=True)) - normed * lax.optimization_barrier(jnp.mean(weighted * normed, -1, keepdims=True)))

def noise_scale(levels):
    sigma_vals = SIGMA_LOW * SIGMA_SPAN ** (levels.astype(jnp.float32) / (LEVELS - 1))
    return lax.rsqrt(1.0 + sigma_vals * sigma_vals)

def reference(pair_repr, pair_mask, chain_id, tri_in_gain, tri_proj, tri_gate, tri_out_gain, tri_out, bias_gain, bias_weight, chain_bias, tokens, noise_level, attn_gain, attn_weight, out_weight, cotangent):
    highest_precision = lax.Precision.HIGHEST
    token_count = pair_repr.shape[0]
    channels = pair_repr.shape[2]
    heads_all = bias_weight.shape[1]
    hidden_width = attn_gain.shape[0]
    head_size = hidden_width // heads_all
    inverse_square_root = 1.0 / jnp.sqrt(jnp.float32(head_size))
    pair_tile = pair_repr.astype(jnp.float32)
    pair_in = (normalize(pair_tile) * tri_in_gain).astype(jnp.bfloat16)
    flat_in = pair_in.reshape(-1, channels)
    projected = jnp.dot(flat_in, tri_proj, preferred_element_type=jnp.float32).reshape(token_count, token_count, 4, channels)
    mask_tile = pair_mask.astype(jnp.float32)[:, :, None]
    left_proj = (jax.nn.sigmoid(projected[:, :, 0]) * projected[:, :, 1] * mask_tile).astype(jnp.bfloat16)
    right_proj = (jax.nn.sigmoid(projected[:, :, 2]) * projected[:, :, 3] * mask_tile).astype(jnp.bfloat16)
    gate_act = jax.nn.sigmoid(jnp.dot(flat_in, tri_gate, preferred_element_type=jnp.float32)).reshape(token_count, token_count, channels)
    triangle = jnp.einsum('ikc,jkc->ijc', left_proj.astype(jnp.float32), right_proj.astype(jnp.float32), precision=highest_precision)
    tri_normed = (normalize(triangle) * tri_out_gain).astype(jnp.bfloat16)
    update = jnp.dot(tri_normed.reshape(-1, channels), tri_out, preferred_element_type=jnp.float32).reshape(token_count, token_count, channels)
    updated = pair_tile + gate_act * update
    bias_in = (normalize(updated) * bias_gain).astype(jnp.bfloat16)
    flat_bias = bias_in.reshape(-1, channels)
    bias_tile = jnp.dot(flat_bias, bias_weight, preferred_element_type=jnp.float32).reshape(token_count, token_count, heads_all)
    same_chain = (chain_id[:, None] == chain_id[None, :]).astype(jnp.float32)
    bias_tile = bias_tile + same_chain[:, :, None] * chain_bias
    per_head_bias = jnp.transpose(bias_tile.astype(jnp.bfloat16), (2, 0, 1)).astype(jnp.float32)
    scales = noise_scale(noise_level)
    weight_f = attn_weight.astype(jnp.float32)

    def one_copy(carried, inputs):
        bias_sums, weight_sums, output_sums = carried
        token_rows, cot_rows, scaling = inputs
        sequence_length = token_rows.shape[0]
        scaled = scaling * token_rows.astype(jnp.float32)
        hidden = (normalize(scaled) * attn_gain).astype(jnp.bfloat16)
        projections = jnp.einsum('nd,gde->gne', hidden.astype(jnp.float32), weight_f, precision=highest_precision)
        query_rows = projections[0].astype(jnp.bfloat16).astype(jnp.float32).reshape(sequence_length, heads_all, head_size)
        key_matrix = projections[1].astype(jnp.bfloat16).astype(jnp.float32).reshape(sequence_length, heads_all, head_size)
        value_rows = projections[2].astype(jnp.bfloat16).astype(jnp.float32).reshape(sequence_length, heads_all, head_size)
        gate_sig = jax.nn.sigmoid(projections[3])
        logit_scores = jnp.einsum('fuc,suc->ufs', query_rows, key_matrix, precision=highest_precision) * inverse_square_root + per_head_bias
        exponent = jnp.exp(logit_scores)
        attention = exponent / lax.optimization_barrier(jnp.sum(exponent, -1, keepdims=True))
        attention_probs = attention.astype(jnp.bfloat16).astype(jnp.float32)
        attended_rows = jnp.einsum('vkq,qvy->kvy', attention_probs, value_rows, precision=highest_precision).reshape(sequence_length, hidden_width)
        gated_out = (gate_sig * attended_rows).astype(jnp.bfloat16)
        attn_out = jnp.dot(gated_out, out_weight, preferred_element_type=jnp.float32)
        denoised = (scaled + attn_out).astype(jnp.bfloat16)
        grad_gated = jnp.dot(cot_rows, out_weight.T, preferred_element_type=jnp.float32)
        grad_gate = grad_gated * attended_rows * gate_sig * (1.0 - gate_sig)
        attended_gradient = (grad_gated * gate_sig).astype(jnp.bfloat16).astype(jnp.float32).reshape(sequence_length, heads_all, head_size)
        probability_gradient = jnp.einsum('fuc,suc->ufs', attended_gradient, value_rows, precision=highest_precision)
        value_gradient = jnp.einsum('avj,vat->jat', attention_probs, attended_gradient, precision=highest_precision)
        grad_score = attention * (probability_gradient - lax.optimization_barrier(jnp.sum(attention * probability_gradient, -1, keepdims=True)))
        score_gradient = grad_score.astype(jnp.bfloat16).astype(jnp.float32)
        query_gradient = jnp.einsum('vkq,qvy->kvy', score_gradient, key_matrix, precision=highest_precision) * inverse_square_root
        key_gradient = jnp.einsum('avj,vat->jat', score_gradient, query_rows, precision=highest_precision) * inverse_square_root
        grads = jnp.stack([query_gradient.reshape(sequence_length, hidden_width), key_gradient.reshape(sequence_length, hidden_width), value_gradient.reshape(sequence_length, hidden_width), grad_gate]).astype(jnp.bfloat16).astype(jnp.float32)
        grad_hidden = jnp.einsum('gne,gde->nd', grads, weight_f, precision=highest_precision)
        grad_scaled = cot_rows.astype(jnp.float32) + norm_back(grad_hidden, scaled, attn_gain)
        token_grad = (scaling * grad_scaled).astype(jnp.bfloat16)
        weight_sums = weight_sums + jnp.einsum('nd,gne->gde', hidden.astype(jnp.float32), grads, precision=highest_precision)
        output_sums = output_sums + jnp.dot(gated_out.T, cot_rows, preferred_element_type=jnp.float32)
        return ((bias_sums + grad_score, weight_sums, output_sums), (denoised, token_grad))
    start_sums = (jnp.zeros((heads_all, token_count, token_count), jnp.float32), jnp.zeros(attn_weight.shape, jnp.float32), jnp.zeros(out_weight.shape, jnp.float32))
    final_sums, stacked = lax.scan(one_copy, start_sums, (tokens, cotangent, scales))
    bias_sums, weight_sums, output_sums = final_sums
    denoised, token_grad = stacked
    grad_bias = jnp.transpose(bias_sums, (1, 2, 0)).reshape(-1, heads_all)
    grad_in = jnp.dot(grad_bias, bias_weight.astype(jnp.float32).T, precision=highest_precision).reshape(token_count, token_count, channels)
    pair_grad = norm_back(grad_in, updated, bias_gain)
    bias_weight_grad = jnp.dot(flat_bias.astype(jnp.float32).T, grad_bias, precision=highest_precision)
    return (updated.astype(jnp.bfloat16), pair_grad, bias_weight_grad, denoised, token_grad, weight_sums, output_sums)
```

```python
import functools
import math

import jax
import jax.numpy as jnp
from jax import lax
from jax.experimental import pallas as pl
from jax.experimental.pallas import tpu as pltpu
from jax.sharding import PartitionSpec as P

LEVELS = 200


EPSILON = 1e-05
SIGMA_LOW = 0.1
SIGMA_SPAN = 100.0


def normalize(values):
    average = jnp.mean(values, -1, keepdims=True)
    centred = values - average
    return centred * lax.rsqrt(jnp.mean(centred * centred, -1, keepdims=True) + EPSILON)


def norm_back(gradient, values, norm_gain):
    average = jnp.mean(values, -1, keepdims=True)
    centred = values - average
    inverse = lax.rsqrt(jnp.mean(centred * centred, -1, keepdims=True) + EPSILON)
    normed = centred * inverse
    weighted = gradient * norm_gain
    return inverse * (
        weighted
        - jnp.mean(weighted, -1, keepdims=True)
        - normed * jnp.mean(weighted * normed, -1, keepdims=True)
    )


def noise_scale(levels):
    sigma_vals = SIGMA_LOW * SIGMA_SPAN ** (levels.astype(jnp.float32) / (LEVELS - 1))
    return lax.rsqrt(1.0 + sigma_vals * sigma_vals)


def general_shards(
    pair_repr,
    pair_mask,
    chain_id,
    tri_in_gain,
    tri_proj,
    tri_gate,
    tri_out_gain,
    tri_out,
    bias_gain,
    bias_weight,
    chain_bias,
    tokens,
    noise_level,
    attn_gain,
    attn_weight,
    out_weight,
    cotangent,
):
    rows_here = pair_repr.shape[0]
    cols_here = pair_repr.shape[1]
    channels = pair_repr.shape[2]
    token_count = chain_id.shape[0]
    heads_all = bias_weight.shape[1]
    hidden_width = attn_gain.shape[0]
    head_size = hidden_width // heads_all
    inverse_square_root = 1.0 / math.sqrt(head_size)
    row_index = lax.axis_index(("group", "row"))
    col_index = lax.axis_index("col")
    pair_tile = pair_repr.astype(jnp.float32)
    pair_in = (normalize(pair_tile) * tri_in_gain).astype(jnp.bfloat16)
    flat_in = pair_in.reshape(-1, channels)
    projected = jnp.dot(flat_in, tri_proj, preferred_element_type=jnp.float32).reshape(
        rows_here, cols_here, 4, channels
    )
    mask_tile = pair_mask.astype(jnp.float32)[:, :, None]
    left_proj = (jax.nn.sigmoid(projected[:, :, 0]) * projected[:, :, 1] * mask_tile).astype(
        jnp.bfloat16
    )
    right_proj = (jax.nn.sigmoid(projected[:, :, 2]) * projected[:, :, 3] * mask_tile).astype(
        jnp.bfloat16
    )
    gate_act = jax.nn.sigmoid(
        jnp.dot(flat_in, tri_gate, preferred_element_type=jnp.float32)
    ).reshape(rows_here, cols_here, channels)
    left_major = jnp.transpose(left_proj, (2, 0, 1))
    right_major = jnp.transpose(right_proj, (2, 0, 1))
    partial_rows = jnp.einsum(
        "cjk,cik->cji",
        lax.all_gather(right_major, ("group", "row"), axis=1, tiled=True),
        left_major,
        preferred_element_type=jnp.float32,
    )
    summed = lax.psum_scatter(partial_rows, "col", scatter_dimension=1, tiled=True)
    triangle = jnp.transpose(summed, (2, 1, 0))
    tri_normed = (normalize(triangle) * tri_out_gain).astype(jnp.bfloat16)
    update = jnp.dot(
        tri_normed.reshape(-1, channels), tri_out, preferred_element_type=jnp.float32
    ).reshape(rows_here, cols_here, channels)
    updated = pair_tile + gate_act * update
    bias_in = (normalize(updated) * bias_gain).astype(jnp.bfloat16)
    flat_bias = bias_in.reshape(-1, channels)
    bias_tile = jnp.dot(flat_bias, bias_weight, preferred_element_type=jnp.float32).reshape(
        rows_here, cols_here, heads_all
    )
    row_chain = lax.dynamic_slice_in_dim(chain_id, row_index * rows_here, rows_here)
    col_chain = lax.dynamic_slice_in_dim(chain_id, col_index * cols_here, cols_here)
    same_chain = (row_chain[:, None] == col_chain[None, :]).astype(jnp.float32)
    bias_tile = bias_tile + same_chain[:, :, None] * chain_bias
    bias_major = jnp.transpose(bias_tile.astype(jnp.bfloat16), (2, 0, 1))
    head_rows = lax.all_to_all(bias_major, "col", split_axis=0, concat_axis=2, tiled=True)
    per_head_bias = lax.all_gather(head_rows, ("group", "row"), axis=1, tiled=True).astype(
        jnp.float32
    )
    local_heads = per_head_bias.shape[0]
    scales = noise_scale(noise_level)

    def one_copy(carried, inputs):
        bias_sums, weight_sums, output_sums = carried
        token_rows, cot_rows, scaling = inputs
        sequence_length = token_rows.shape[0]
        scaled = scaling * token_rows.astype(jnp.float32)
        hidden = (normalize(scaled) * attn_gain).astype(jnp.bfloat16)
        projections = jnp.einsum(
            "nd,gde->gne", hidden, attn_weight, preferred_element_type=jnp.float32
        )
        query_rows = (
            projections[0].astype(jnp.bfloat16).reshape(sequence_length, local_heads, head_size)
        )
        key_matrix = (
            projections[1].astype(jnp.bfloat16).reshape(sequence_length, local_heads, head_size)
        )
        value_rows = (
            projections[2].astype(jnp.bfloat16).reshape(sequence_length, local_heads, head_size)
        )
        gate_sig = jax.nn.sigmoid(projections[3])
        logit_scores = (
            jnp.einsum("fuc,suc->ufs", query_rows, key_matrix, preferred_element_type=jnp.float32)
            * inverse_square_root
            + per_head_bias
        )
        exponent = jnp.exp(logit_scores)
        attention = exponent / jnp.sum(exponent, -1, keepdims=True)
        attention_probs = attention.astype(jnp.bfloat16)
        attended_rows = jnp.einsum(
            "vkq,qvy->kvy", attention_probs, value_rows, preferred_element_type=jnp.float32
        ).reshape(sequence_length, -1)
        gated_out = (gate_sig * attended_rows).astype(jnp.bfloat16)
        grad_gated = jnp.dot(cot_rows, out_weight.T, preferred_element_type=jnp.float32)
        grad_gate = grad_gated * attended_rows * gate_sig * (1.0 - gate_sig)
        attended_gradient = (
            (grad_gated * gate_sig)
            .astype(jnp.bfloat16)
            .reshape(sequence_length, local_heads, head_size)
        )
        probability_gradient = jnp.einsum(
            "fuc,suc->ufs", attended_gradient, value_rows, preferred_element_type=jnp.float32
        )
        value_gradient = jnp.einsum(
            "avj,vat->jat", attention_probs, attended_gradient, preferred_element_type=jnp.float32
        )
        grad_score = attention * (
            probability_gradient - jnp.sum(attention * probability_gradient, -1, keepdims=True)
        )
        score_gradient = grad_score.astype(jnp.bfloat16)
        query_gradient = (
            jnp.einsum(
                "vkq,qvy->kvy", score_gradient, key_matrix, preferred_element_type=jnp.float32
            )
            * inverse_square_root
        )
        key_gradient = (
            jnp.einsum(
                "avj,vat->jat", score_gradient, query_rows, preferred_element_type=jnp.float32
            )
            * inverse_square_root
        )
        grads = jnp.stack(
            [
                query_gradient.reshape(sequence_length, -1),
                key_gradient.reshape(sequence_length, -1),
                value_gradient.reshape(sequence_length, -1),
                grad_gate,
            ]
        ).astype(jnp.bfloat16)
        weight_sums = weight_sums + jnp.einsum(
            "nd,gne->gde", hidden, grads, preferred_element_type=jnp.float32
        )
        output_sums = output_sums + jnp.dot(
            gated_out.T, cot_rows, preferred_element_type=jnp.float32
        )
        return ((bias_sums + grad_score, weight_sums, output_sums), (gated_out, grads))

    start_sums = (
        jnp.zeros((local_heads, token_count, token_count), jnp.float32),
        jnp.zeros(attn_weight.shape, jnp.float32),
        jnp.zeros(out_weight.shape, jnp.float32),
    )
    final_sums, stacked = lax.scan(one_copy, start_sums, (tokens, cotangent, scales))
    bias_sums, weight_sums, output_sums = final_sums
    gated_all, grads_all = stacked
    token_share = token_count // lax.axis_size("col")
    attn_parts = jnp.einsum(
        "tnd,de->tne", gated_all, out_weight, preferred_element_type=jnp.float32
    )
    hidden_parts = jnp.einsum(
        "tgne,gde->tnd", grads_all, attn_weight, preferred_element_type=jnp.float32
    )
    attn_out, grad_hidden = (
        lax.psum_scatter(attn_parts, "col", scatter_dimension=1, tiled=True),
        lax.psum_scatter(hidden_parts, "col", scatter_dimension=1, tiled=True),
    )
    first_token = col_index * token_share
    token_mine = lax.dynamic_slice_in_dim(tokens, first_token, token_share, 1)
    cot_mine = lax.dynamic_slice_in_dim(cotangent, first_token, token_share, 1)
    scaled_mine = scales[:, None, None] * token_mine.astype(jnp.float32)
    denoised = (scaled_mine + attn_out).astype(jnp.bfloat16)
    grad_scaled = cot_mine.astype(jnp.float32) + norm_back(grad_hidden, scaled_mine, attn_gain)
    token_grad = (scales[:, None, None] * grad_scaled).astype(jnp.bfloat16)
    bias_rows_sum, out_grad, weight_grad = (
        lax.psum_scatter(bias_sums, ("group", "row"), scatter_dimension=1, tiled=True),
        lax.psum_scatter(output_sums, ("group", "row"), scatter_dimension=1, tiled=True),
        lax.psum_scatter(weight_sums, ("group", "row"), scatter_dimension=1, tiled=True),
    )
    bias_back = lax.all_to_all(bias_rows_sum, "col", split_axis=2, concat_axis=0, tiled=True)
    grad_bias = jnp.transpose(bias_back, (1, 2, 0)).reshape(-1, heads_all)
    grad_in = jnp.dot(
        grad_bias, bias_weight.astype(jnp.float32).T, precision=lax.Precision.HIGHEST
    ).reshape(rows_here, cols_here, channels)
    pair_grad = norm_back(grad_in, updated, bias_gain)
    weight_part = jnp.dot(
        flat_bias.astype(jnp.float32).T, grad_bias, precision=lax.Precision.HIGHEST
    )
    bias_weight_grad = lax.psum(weight_part, ("group", "row", "col"))
    return (
        updated.astype(jnp.bfloat16),
        pair_grad,
        bias_weight_grad,
        denoised,
        token_grad,
        weight_grad,
        out_grad,
    )


LANES = 128


def dot_nn(a, b, **kw):
    return lax.dot_general(a, b, (((1,), (0,)), ((), ())), preferred_element_type=jnp.float32, **kw)


def dot_nt(a, b, **kw):
    return lax.dot_general(a, b, (((1,), (1,)), ((), ())), preferred_element_type=jnp.float32, **kw)


def dot_tn(a, b, **kw):
    return lax.dot_general(a, b, (((0,), (0,)), ((), ())), preferred_element_type=jnp.float32, **kw)


def turn(values, groups, width):
    shift = (groups * width) % LANES
    return values if shift == 0 else pltpu.roll(values, shift, 1)


def merge(pieces, lane_group):
    merged = pieces[0]
    for g in range(1, len(pieces)):
        merged = jnp.where(lane_group == g, pieces[g], merged)
    return merged


def lane_groups(rows, width):
    return lax.broadcasted_iota(jnp.int32, (rows, LANES), 1) // width


def channel_order(channels, devices):
    r = lax.broadcasted_iota(jnp.int32, (channels, channels), 0)
    c = lax.broadcasted_iota(jnp.int32, (channels, channels), 1)
    return (r % devices) * (channels // devices) + r // devices == c


def whole(shape, dtype):
    return jax.ShapeDtypeStruct(shape, dtype)


def pair_in_kernel(pair_ref, aux_ref, gain_ref, proj_ref, out_ref, rows_ref, *, rows, width):
    devices = out_ref.shape[0]
    channels = pair_ref.shape[1]
    groups = LANES // width
    pair_in = (normalize(pair_ref[...].astype(jnp.float32)) * gain_ref[...]).astype(jnp.bfloat16)
    order = channel_order(channels, devices).astype(jnp.float32).astype(jnp.bfloat16)
    lanes = lane_groups(devices, width)
    for side in range(2):
        first = 2 * side * channels
        gate_t = dot_nt(order, proj_ref[:, first : first + channels]).astype(jnp.bfloat16)
        value_t = dot_nt(order, proj_ref[:, first + channels : first + 2 * channels]).astype(
            jnp.bfloat16
        )
        product = (
            jax.nn.sigmoid(dot_nt(gate_t, pair_in)) * dot_nt(value_t, pair_in) * aux_ref[0:1, :]
        )
        for i in range(rows):
            q, s = divmod(i, groups)
            rows_ref[pl.ds(i, devices, stride=rows), :] = merge(
                [
                    turn(
                        product[g * devices : (g + 1) * devices, q * LANES : (q + 1) * LANES],
                        g - s,
                        width,
                    )
                    for g in range(groups)
                ],
                lanes,
            )
        out_ref[:, side] = rows_ref[...].astype(jnp.bfloat16).reshape(devices, rows, LANES)


def triangle_kernel(in_ref, out_ref, *, width):
    stripes, cols, _, rows, _ = in_ref.shape
    groups = LANES // width
    tokens = stripes * rows
    lanes = lane_groups(tokens, width)
    totals = [jnp.zeros((tokens, LANES), jnp.float32) for _ in range(groups)]
    for col in range(cols):
        left = in_ref[:, col, 0].reshape(tokens, LANES)
        right = in_ref[:, col, 1].reshape(tokens, LANES)
        for g in range(groups):
            totals[g] += dot_nt(jnp.where(lanes == g, left, jnp.zeros_like(left)), right)
    for col in range(cols):
        out_ref[:, col] = (
            merge([turn(totals[g], g - col, width) for g in range(groups)], lanes)
            .astype(jnp.bfloat16)
            .reshape(stripes, rows, LANES)
        )


def pair_out_kernel(
    in_ref,
    pair_ref,
    aux_ref,
    in_gain_ref,
    gate_ref,
    out_gain_ref,
    out_weight_ref,
    bias_gain_ref,
    bias_weight_ref,
    chain_bias_ref,
    next_ref,
    updated_ref,
    bias_ref,
    rows_ref,
    *,
    width,
):
    devices, rows, _ = in_ref.shape
    stripes, cols = bias_ref.shape[:2]
    channels = pair_ref.shape[1]
    heads = bias_weight_ref.shape[1]
    groups = LANES // width

    def all_lanes(sums):
        total = sums
        for g in range(1, groups):
            total = total + turn(sums, g, width)
        return total

    triangle = in_ref[...].astype(jnp.float32)
    average = all_lanes(jnp.sum(triangle, 0)) * (1.0 / channels)
    centred = triangle - average
    inverse = lax.rsqrt(all_lanes(jnp.sum(centred * centred, 0)) * (1.0 / channels) + EPSILON)
    rows_ref[...] = (centred * inverse).reshape(devices * rows, LANES)
    lanes = lane_groups(devices, width)
    blocks = []
    for q in range(rows // groups):
        tiles = [
            rows_ref[pl.ds(q * groups + s, devices, stride=rows), :] for s in range(groups)
        ]
        blocks.append(
            jnp.concatenate(
                [
                    merge([turn(tiles[s], s - g, width) for s in range(groups)], lanes)
                    for g in range(groups)
                ],
                axis=0,
            )
        )
    normed_t = jnp.concatenate(blocks, axis=1)
    order = channel_order(channels, devices)
    gain_t = jnp.sum(jnp.where(order, out_gain_ref[...], 0.0), axis=1, keepdims=True)
    order_b = order.astype(jnp.float32).astype(jnp.bfloat16)
    weight = dot_nn(order_b, out_weight_ref[...]).astype(jnp.bfloat16)
    update = dot_tn((normed_t * gain_t).astype(jnp.bfloat16), weight)
    pair = pair_ref[...].astype(jnp.float32)
    pair_in = (normalize(pair) * in_gain_ref[...]).astype(jnp.bfloat16)
    updated = pair + jax.nn.sigmoid(dot_nn(pair_in, gate_ref[...])) * update
    updated_ref[...] = updated
    next_ref[...] = updated.astype(jnp.bfloat16)
    bias_in = (normalize(updated) * bias_gain_ref[...]).astype(jnp.bfloat16)
    unit = lax.broadcasted_iota(jnp.int32, (heads, heads), 0) == lax.broadcasted_iota(
        jnp.int32, (heads, heads), 1
    )
    chain_t = jnp.sum(jnp.where(unit, chain_bias_ref[...], 0.0), axis=1, keepdims=True)
    bias_weight_t = dot_nt(
        unit.astype(jnp.float32).astype(jnp.bfloat16), bias_weight_ref[...]
    ).astype(jnp.bfloat16)
    bias_t = dot_nt(bias_weight_t, bias_in) + aux_ref[1:2, :] * chain_t
    lanes_h = lane_groups(heads, width)
    head_group = lax.broadcasted_iota(jnp.int32, (heads, LANES), 0) % groups
    spread = []
    for i in range(rows):
        q, s = divmod(i, groups)
        block = bias_t[:, q * LANES : (q + 1) * LANES]
        tile = jnp.zeros_like(block)
        for g in range(groups):
            tile = jnp.where(
                (lanes_h == g) & (head_group == g), turn(block, g - s, width), tile
            )
        spread.append(tile)
    spread = jnp.concatenate(spread, axis=0).astype(jnp.bfloat16)
    packed = dot_nn(head_gather(rows, cols, heads).astype(jnp.bfloat16), spread)
    packed = packed.astype(jnp.bfloat16).reshape(cols, rows, LANES)
    for stripe in range(stripes):
        bias_ref[stripe] = packed


def head_gather(rows, cols, heads):
    a = lax.broadcasted_iota(jnp.int32, (cols * rows, rows * heads), 0)
    b = lax.broadcasted_iota(jnp.int32, (cols * rows, rows * heads), 1)
    return ((a % rows == b // heads) & (a // rows == (b % heads) // (heads // cols))).astype(
        jnp.float32
    )


def token_in_kernel(
    scale_ref,
    tokens_ref,
    cot_ref,
    gain_ref,
    weight_ref,
    out_weight_ref,
    hidden_ref,
    query_ref,
    key_ref,
    value_ref,
    gated_ref,
    sig_ref,
    grad_ref,
):
    copies, length, _ = tokens_ref.shape
    for t in range(copies):
        part = slice(t * length, (t + 1) * length)
        scaled = scale_ref[t] * tokens_ref[t].astype(jnp.float32)
        hidden_ref[part] = (normalize(scaled) * gain_ref[...]).astype(jnp.bfloat16)
    hidden = hidden_ref[...]
    query_ref[...] = dot_nn(hidden, weight_ref[0]).astype(jnp.bfloat16)
    key_ref[...] = dot_nn(hidden, weight_ref[1]).astype(jnp.bfloat16)
    value_ref[...] = dot_nn(hidden, weight_ref[2]).astype(jnp.bfloat16)
    sig = jax.nn.sigmoid(dot_nn(hidden, weight_ref[3]))
    sig_ref[...] = sig
    grad = dot_nt(cot_ref[...].reshape(copies * length, -1), out_weight_ref[...])
    grad_ref[...] = grad
    gated_ref[...] = (grad * sig).astype(jnp.bfloat16)


def attention_kernel(
    col_ref,
    bias_ref,
    hidden_ref,
    query_ref,
    key_ref,
    value_ref,
    gated_ref,
    sig_ref,
    grad_ref,
    cot_ref,
    weight_ref,
    out_weight_ref,
    pair_ref,
    wire_ref,
    *refs,
    width,
    head_size,
):
    part_refs, (sums_ref, parts_ref, outs_ref, grads_ref) = refs[:-4], refs[-4:]
    stripes, cols, rows, _ = bias_ref.shape
    copies, length, hidden_width = cot_ref.shape
    groups = LANES // width
    inner = query_ref.shape[1]
    share = length // cols
    lanes = lane_groups(length, width)
    head_of = lax.broadcasted_iota(jnp.int32, (length, inner), 1) // head_size
    inverse_square_root = 1.0 / math.sqrt(head_size)
    tiles = [
        bias_ref[:, col].astype(jnp.float32).reshape(length, LANES) for col in range(cols)
    ]
    bias = [
        merge([turn(tiles[col], col - h, width) for col in range(cols)], lanes)
        for h in range(groups)
    ]
    for t in range(copies):
        part = slice(t * length, (t + 1) * length)
        query, key_rows, value, gated = (
            r[part] for r in (query_ref, key_ref, value_ref, gated_ref)
        )
        attended = jnp.zeros((length, inner), jnp.float32)
        grad_query, grad_key, grad_value = attended, attended, attended
        for h in range(groups):
            mine = head_of == h
            query_h, key_h, value_h, gated_h = (
                jnp.where(mine, r, jnp.zeros_like(r)) for r in (query, key_rows, value, gated)
            )
            exponent = jnp.exp(dot_nt(query_h, key_rows) * inverse_square_root + bias[h])
            attention = exponent / jnp.sum(exponent, -1, keepdims=True)
            attention_b = attention.astype(jnp.bfloat16)
            grad_prob = dot_nt(gated_h, value)
            grad_score = attention * (
                grad_prob - jnp.sum(attention * grad_prob, -1, keepdims=True)
            )
            sums_ref[h] = grad_score if t == 0 else sums_ref[h] + grad_score
            score_b = grad_score.astype(jnp.bfloat16)
            attended += dot_nn(attention_b, value_h)
            grad_query += dot_nn(score_b, key_h)
            grad_key += dot_tn(score_b, query_h)
            grad_value += dot_tn(attention_b, gated_h)
        sig = sig_ref[part]
        gated_out = (sig * attended).astype(jnp.bfloat16)
        grads = [
            (grad_query * inverse_square_root).astype(jnp.bfloat16),
            (grad_key * inverse_square_root).astype(jnp.bfloat16),
            grad_value.astype(jnp.bfloat16),
            (grad_ref[part] * attended * sig * (1.0 - sig)).astype(jnp.bfloat16),
        ]
        outs_ref[part] = gated_out
        for g in range(4):
            grads_ref[g, part] = grads[g]
        out_part = dot_nn(gated_out, out_weight_ref[...])
        in_part = dot_nt(grads[0], weight_ref[0])
        for g in range(1, 4):
            in_part += dot_nt(grads[g], weight_ref[g])
        parts_ref[:, 0, t] = out_part.astype(jnp.bfloat16).reshape(cols, share, hidden_width)
        parts_ref[:, 1, t] = in_part.astype(jnp.bfloat16).reshape(cols, share, hidden_width)
    for k in range(cols):
        part_refs[k][...] = parts_ref[(col_ref[0] + k) % cols]
    for col in range(cols):
        pair_ref[:, col] = (
            merge([turn(sums_ref[h], h - col, width) for h in range(groups)], lanes)
            .astype(jnp.bfloat16)
            .reshape(stripes, rows, LANES)
        )
    hidden = hidden_ref[...]
    weights = [dot_tn(hidden, grads_ref[g]) for g in range(4)]
    weights.append(dot_tn(cot_ref[...].reshape(copies * length, hidden_width), outs_ref[...]))
    for g in range(5):
        wire_ref[:, g * LANES : (g + 1) * LANES] = weights[g][:, :LANES].astype(jnp.bfloat16)
    tails = [w[:, LANES:] for w in weights]
    tails.append(jnp.zeros_like(tails[0]))
    for g in range(3):
        wire_ref[:, (5 + g) * LANES : (6 + g) * LANES] = jnp.concatenate(
            tails[2 * g : 2 * g + 2], axis=1
        ).astype(jnp.bfloat16)


def pair_back_kernel(
    in_ref, updated_ref, gain_ref, bias_weight_ref, grad_ref, weight_ref, *, width
):
    stripes, cols, rows, _ = in_ref.shape
    heads = bias_weight_ref.shape[1]
    groups = LANES // width
    total = jnp.sum(in_ref[...].astype(jnp.float32), 0).reshape(cols * rows, LANES)
    spread = dot_tn(head_gather(rows, cols, heads), total, precision=lax.Precision.HIGHEST)
    lanes = lane_groups(heads, width)
    head_group = lax.broadcasted_iota(jnp.int32, (heads, LANES), 0) % groups
    blocks = []
    for q in range(rows // groups):
        tiles = []
        for s in range(groups):
            i = q * groups + s
            tile = spread[i * heads : (i + 1) * heads]
            turned = tile
            for g in range(groups):
                turned = jnp.where(head_group == g, turn(tile, s - g, width), turned)
            tiles.append(turned)
        blocks.append(merge(tiles, lanes))
    grad_t = jnp.concatenate(blocks, axis=1)
    updated = updated_ref[...]
    gain = gain_ref[...]
    grad_in = lax.dot_general(
        grad_t,
        bias_weight_ref[...].astype(jnp.float32),
        (((0,), (1,)), ((), ())),
        precision=lax.Precision.HIGHEST,
        preferred_element_type=jnp.float32,
    )
    grad_ref[...] = norm_back(grad_in, updated, gain)
    bias_in = (normalize(updated) * gain).astype(jnp.bfloat16).astype(jnp.float32)
    weight = dot_nn(grad_t, bias_in, precision=lax.Precision.HIGHEST).astype(jnp.bfloat16)
    for device in range(weight_ref.shape[0]):
        weight_ref[device] = weight


def token_out_kernel(
    col_ref, scale_ref, tokens_ref, cot_ref, gain_ref, *refs
):
    part_refs, (out_ref, grad_ref) = refs[:-2], refs[-2:]
    for t in range(out_ref.shape[0]):
        sums = part_refs[0][:, t].astype(jnp.float32)
        for r in part_refs[1:]:
            sums = sums + r[:, t].astype(jnp.float32)
        scale = scale_ref[t]
        scaled = scale * tokens_ref[t].astype(jnp.float32)
        out_ref[t] = (scaled + sums[0]).astype(jnp.bfloat16)
        grad = cot_ref[t].astype(jnp.float32) + norm_back(sums[1], scaled, gain_ref[...])
        grad_ref[t] = (scale * grad).astype(jnp.bfloat16)


def weight_out_kernel(in_ref, grad_ref, out_ref):
    total = jnp.sum(in_ref[...].astype(jnp.float32), 0)
    half = LANES // 2
    for g in range(4):
        grad_ref[g, :, :LANES] = total[:, g * LANES : (g + 1) * LANES]
        first = (5 + g // 2) * LANES + (g % 2) * half
        grad_ref[g, :, LANES:] = total[:, first : first + half]
    rows = jnp.concatenate(
        [total[:, 4 * LANES : 5 * LANES], total[:, 7 * LANES : 8 * LANES]], axis=1
    )
    out_ref[...] = rows.T[: out_ref.shape[0]]


def fits(pair_repr, token_count, heads_all, inner, hidden_width, stripes, cols):
    rows, width, channels = pair_repr.shape
    groups = LANES // width if LANES % width == 0 else 0
    return (
        groups > 0
        and token_count == LANES
        and channels == LANES
        and channels == stripes * cols * groups
        and cols == groups
        and heads_all == cols * groups
        and rows % 16 == 0
        and stripes * rows == token_count
        and inner == LANES + LANES // 2
        and hidden_width % (16 * stripes) == 0
    )


def shards(
    pair_repr,
    pair_mask,
    chain_id,
    tri_in_gain,
    tri_proj,
    tri_gate,
    tri_out_gain,
    tri_out,
    bias_gain,
    bias_weight,
    chain_bias,
    tokens,
    noise_level,
    attn_gain,
    attn_weight,
    out_weight,
    cotangent,
):
    stripe_axes = ("group", "row")
    all_axes = ("group", "row", "col")
    stripes = lax.axis_size(stripe_axes)
    cols = lax.axis_size("col")
    rows, width, channels = pair_repr.shape
    heads_all = bias_weight.shape[1]
    copies, length, hidden_width = tokens.shape
    inner = attn_weight.shape[2]
    if not fits(pair_repr, length, heads_all, inner, hidden_width, stripes, cols):
        return general_shards(
            pair_repr,
            pair_mask,
            chain_id,
            tri_in_gain,
            tri_proj,
            tri_gate,
            tri_out_gain,
            tri_out,
            bias_gain,
            bias_weight,
            chain_bias,
            tokens,
            noise_level,
            attn_gain,
            attn_weight,
            out_weight,
            cotangent,
        )
    head_size = hidden_width // heads_all
    devices = stripes * cols
    pairs = rows * width
    bf16, f32 = jnp.bfloat16, jnp.float32
    vmem = pl.BlockSpec(memory_space=pltpu.VMEM)
    smem = pl.BlockSpec(memory_space=pltpu.SMEM)
    row_index = lax.axis_index(stripe_axes)
    col_index = lax.axis_index("col")
    here = jnp.reshape(col_index, (1,)).astype(jnp.int32)
    row_chain = lax.dynamic_slice_in_dim(chain_id, row_index * rows, rows)
    col_chain = lax.dynamic_slice_in_dim(chain_id, col_index * width, width)
    same_chain = (row_chain[:, None] == col_chain[None, :]).astype(f32)
    aux = jnp.stack([pair_mask.astype(f32), same_chain]).reshape(2, pairs)
    pair_flat = pair_repr.reshape(pairs, channels)
    scales = noise_scale(noise_level)

    projected = pl.pallas_call(
        functools.partial(pair_in_kernel, rows=rows, width=width),
        out_shape=whole((devices, 2, rows, LANES), bf16),
        in_specs=[vmem] * 4,
        out_specs=vmem,
        scratch_shapes=[pltpu.VMEM((devices * rows, LANES), f32)],
        name="pair_in",
    )(pair_flat, aux, tri_in_gain[None], tri_proj)
    sides = lax.all_to_all(
        projected.reshape(devices, 2 * rows, LANES), all_axes, 0, 0, tiled=True
    )
    hidden, query, key_rows, value, gated, gate_sig, grad_gated = pl.pallas_call(
        token_in_kernel,
        out_shape=(
            whole((copies * length, hidden_width), bf16),
            *[whole((copies * length, inner), bf16)] * 4,
            *[whole((copies * length, inner), f32)] * 2,
        ),
        in_specs=[smem] + [vmem] * 5,
        out_specs=(vmem,) * 7,
        name="token_in",
    )(scales, tokens, cotangent, attn_gain[None], attn_weight, out_weight)
    triangle = pl.pallas_call(
        functools.partial(triangle_kernel, width=width),
        out_shape=whole((stripes, cols, rows, LANES), bf16),
        in_specs=[vmem],
        out_specs=vmem,
        name="triangle",
    )(sides.reshape(stripes, cols, 2, rows, LANES))
    triangle = lax.all_to_all(
        triangle.reshape(devices, rows, LANES), all_axes, 0, 0, tiled=True
    )
    pair_next, updated, bias_tile = pl.pallas_call(
        functools.partial(pair_out_kernel, width=width),
        out_shape=(
            whole((pairs, channels), bf16),
            whole((pairs, channels), f32),
            whole((stripes, cols, rows, LANES), bf16),
        ),
        in_specs=[vmem] * 10,
        out_specs=(vmem,) * 3,
        scratch_shapes=[pltpu.VMEM((devices * rows, LANES), f32)],
        name="pair_out",
    )(
        triangle,
        pair_flat,
        aux,
        tri_in_gain[None],
        tri_gate,
        tri_out_gain[None],
        tri_out,
        bias_gain[None],
        bias_weight,
        chain_bias[None],
    )
    head_bias = lax.all_to_all(
        bias_tile.reshape(devices, rows, LANES), all_axes, 0, 0, tiled=True
    )
    part = whole((2, copies, length // cols, hidden_width), bf16)
    bias_sums, wire, *parts = pl.pallas_call(
        functools.partial(attention_kernel, width=width, head_size=head_size),
        out_shape=(
            whole((stripes, cols, rows, LANES), bf16),
            whole((hidden_width, 8 * LANES), bf16),
            *[part] * cols,
        ),
        in_specs=[smem] + [vmem] * 11,
        out_specs=(vmem,) * (2 + cols),
        scratch_shapes=[
            pltpu.VMEM((LANES // width, length, LANES), f32),
            pltpu.VMEM((cols,) + part.shape, bf16),
            pltpu.VMEM((copies * length, inner), bf16),
            pltpu.VMEM((4, copies * length, inner), bf16),
        ],
        name="attention",
    )(
        here,
        head_bias.reshape(stripes, cols, rows, LANES),
        hidden,
        query,
        key_rows,
        value,
        gated,
        gate_sig,
        grad_gated,
        cotangent,
        attn_weight,
        out_weight,
    )
    bias_back = lax.all_to_all(
        bias_sums.reshape(devices, rows, LANES), all_axes, 0, 0, tiled=True
    )
    *parts, bias_back, wire = lax.optimization_barrier((*parts, bias_back, wire))
    received = [parts[0]] + [
        lax.ppermute(parts[k], "col", [(i, (i + k) % cols) for i in range(cols)])
        for k in range(1, cols)
    ]
    pair_grad, weight_part = pl.pallas_call(
        functools.partial(pair_back_kernel, width=width),
        out_shape=(whole((pairs, channels), f32), whole((devices, heads_all, channels), bf16)),
        in_specs=[vmem] * 4,
        out_specs=(vmem,) * 2,
        name="pair_back",
    )(bias_back.reshape(stripes, cols, rows, LANES), updated, bias_gain[None], bias_weight)
    wire = lax.all_to_all(
        wire.reshape(stripes, hidden_width // stripes, 8 * LANES), stripe_axes, 0, 0, tiled=True
    )
    weight_grad, out_grad = pl.pallas_call(
        weight_out_kernel,
        out_shape=(
            whole((4, hidden_width // stripes, inner), f32),
            whole((inner, hidden_width // stripes), f32),
        ),
        in_specs=[vmem],
        out_specs=(vmem,) * 2,
        name="weight_out",
    )(wire)
    weight_part = lax.all_to_all(weight_part, all_axes, 0, 0, tiled=True)
    bias_weight_grad = jnp.sum(weight_part.astype(f32), 0).T
    share = length // cols
    mine = pl.BlockSpec((copies, share, hidden_width), lambda i, col: (0, col[0], 0))
    fixed = lambda shape: pl.BlockSpec(shape, lambda i, col: (0,) * len(shape))
    denoised, token_grad = pl.pallas_call(
        token_out_kernel,
        grid_spec=pltpu.PrefetchScalarGridSpec(
            num_scalar_prefetch=1,
            grid=(1,),
            in_specs=[smem, mine, mine, fixed((1, hidden_width))] + [fixed(part.shape)] * cols,
            out_specs=[fixed((copies, share, hidden_width))] * 2,
        ),
        out_shape=(whole((copies, share, hidden_width), bf16),) * 2,
        name="token_out",
    )(here, scales, tokens, cotangent, attn_gain[None], *received)
    return (
        pair_next.reshape(rows, width, channels),
        pair_grad.reshape(rows, width, channels),
        bias_weight_grad,
        denoised,
        token_grad,
        weight_grad,
        out_grad,
    )


def solution(mesh):
    return jax.shard_map(
        shards,
        mesh=mesh,
        in_specs=(
            P(("group", "row"), "col", None),
            P(("group", "row"), "col"),
            P(),
            P(),
            P(),
            P(),
            P(),
            P(),
            P(),
            P(),
            P(),
            P(("group", "row"), None, None),
            P(("group", "row")),
            P(),
            P(None, None, "col"),
            P("col", None),
            P(("group", "row"), None, None),
        ),
        out_specs=(
            P(("group", "row"), "col", None),
            P(("group", "row"), "col", None),
            P(),
            P(("group", "row"), "col", None),
            P(("group", "row"), "col", None),
            P(None, ("group", "row"), "col"),
            P("col", ("group", "row")),
        ),
        check_vma=False,
    )
```

```python
import functools
import math

import jax
import jax.numpy as jnp
from jax import lax
from jax.experimental import pallas as pl
from jax.experimental.pallas import tpu as pltpu
from jax.sharding import PartitionSpec as P


LEVELS = 200


EPSILON = 1e-05
SIGMA_LOW = 0.1
SIGMA_SPAN = 100.0


def normalize(values):
    average = jnp.mean(values, -1, keepdims=True)
    centred = values - average
    return centred * lax.rsqrt(jnp.mean(centred * centred, -1, keepdims=True) + EPSILON)


def norm_back(gradient, values, norm_gain):
    average = jnp.mean(values, -1, keepdims=True)
    centred = values - average
    inverse = lax.rsqrt(jnp.mean(centred * centred, -1, keepdims=True) + EPSILON)
    normed = centred * inverse
    weighted = gradient * norm_gain
    return inverse * (
        weighted
        - jnp.mean(weighted, -1, keepdims=True)
        - normed * jnp.mean(weighted * normed, -1, keepdims=True)
    )


def noise_scale(levels):
    sigma_vals = SIGMA_LOW * SIGMA_SPAN ** (levels.astype(jnp.float32) / (LEVELS - 1))
    return lax.rsqrt(1.0 + sigma_vals * sigma_vals)


def general_shards(
    pair_repr,
    pair_mask,
    chain_id,
    tri_in_gain,
    tri_proj,
    tri_gate,
    tri_out_gain,
    tri_out,
    bias_gain,
    bias_weight,
    chain_bias,
    tokens,
    noise_level,
    attn_gain,
    attn_weight,
    out_weight,
    cotangent,
):
    rows_here = pair_repr.shape[0]
    cols_here = pair_repr.shape[1]
    channels = pair_repr.shape[2]
    token_count = chain_id.shape[0]
    heads_all = bias_weight.shape[1]
    hidden_width = attn_gain.shape[0]
    head_size = hidden_width // heads_all
    inverse_square_root = 1.0 / math.sqrt(head_size)
    row_index = lax.axis_index(("group", "row"))
    col_index = lax.axis_index("col")
    pair_tile = pair_repr.astype(jnp.float32)
    pair_in = (normalize(pair_tile) * tri_in_gain).astype(jnp.bfloat16)
    flat_in = pair_in.reshape(-1, channels)
    projected = jnp.dot(flat_in, tri_proj, preferred_element_type=jnp.float32).reshape(
        rows_here, cols_here, 4, channels
    )
    mask_tile = pair_mask.astype(jnp.float32)[:, :, None]
    left_proj = (jax.nn.sigmoid(projected[:, :, 0]) * projected[:, :, 1] * mask_tile).astype(
        jnp.bfloat16
    )
    right_proj = (jax.nn.sigmoid(projected[:, :, 2]) * projected[:, :, 3] * mask_tile).astype(
        jnp.bfloat16
    )
    gate_act = jax.nn.sigmoid(
        jnp.dot(flat_in, tri_gate, preferred_element_type=jnp.float32)
    ).reshape(rows_here, cols_here, channels)
    left_major = jnp.transpose(left_proj, (2, 0, 1))
    right_major = jnp.transpose(right_proj, (2, 0, 1))
    partial_rows = jnp.einsum(
        "cjk,cik->cji",
        lax.all_gather(right_major, ("group", "row"), axis=1, tiled=True),
        left_major,
        preferred_element_type=jnp.float32,
    )
    summed = lax.psum_scatter(partial_rows, "col", scatter_dimension=1, tiled=True)
    triangle = jnp.transpose(summed, (2, 1, 0))
    tri_normed = (normalize(triangle) * tri_out_gain).astype(jnp.bfloat16)
    update = jnp.dot(
        tri_normed.reshape(-1, channels), tri_out, preferred_element_type=jnp.float32
    ).reshape(rows_here, cols_here, channels)
    updated = pair_tile + gate_act * update
    bias_in = (normalize(updated) * bias_gain).astype(jnp.bfloat16)
    flat_bias = bias_in.reshape(-1, channels)
    bias_tile = jnp.dot(flat_bias, bias_weight, preferred_element_type=jnp.float32).reshape(
        rows_here, cols_here, heads_all
    )
    row_chain = lax.dynamic_slice_in_dim(chain_id, row_index * rows_here, rows_here)
    col_chain = lax.dynamic_slice_in_dim(chain_id, col_index * cols_here, cols_here)
    same_chain = (row_chain[:, None] == col_chain[None, :]).astype(jnp.float32)
    bias_tile = bias_tile + same_chain[:, :, None] * chain_bias
    bias_major = jnp.transpose(bias_tile.astype(jnp.bfloat16), (2, 0, 1))
    head_rows = lax.all_to_all(bias_major, "col", split_axis=0, concat_axis=2, tiled=True)
    per_head_bias = lax.all_gather(head_rows, ("group", "row"), axis=1, tiled=True).astype(
        jnp.float32
    )
    local_heads = per_head_bias.shape[0]
    scales = noise_scale(noise_level)

    def one_copy(carried, inputs):
        bias_sums, weight_sums, output_sums = carried
        token_rows, cot_rows, scaling = inputs
        sequence_length = token_rows.shape[0]
        scaled = scaling * token_rows.astype(jnp.float32)
        hidden = (normalize(scaled) * attn_gain).astype(jnp.bfloat16)
        projections = jnp.einsum(
            "nd,gde->gne", hidden, attn_weight, preferred_element_type=jnp.float32
        )
        query_rows = (
            projections[0].astype(jnp.bfloat16).reshape(sequence_length, local_heads, head_size)
        )
        key_matrix = (
            projections[1].astype(jnp.bfloat16).reshape(sequence_length, local_heads, head_size)
        )
        value_rows = (
            projections[2].astype(jnp.bfloat16).reshape(sequence_length, local_heads, head_size)
        )
        gate_sig = jax.nn.sigmoid(projections[3])
        logit_scores = (
            jnp.einsum("fuc,suc->ufs", query_rows, key_matrix, preferred_element_type=jnp.float32)
            * inverse_square_root
            + per_head_bias
        )
        exponent = jnp.exp(logit_scores)
        attention = exponent / jnp.sum(exponent, -1, keepdims=True)
        attention_probs = attention.astype(jnp.bfloat16)
        attended_rows = jnp.einsum(
            "vkq,qvy->kvy", attention_probs, value_rows, preferred_element_type=jnp.float32
        ).reshape(sequence_length, -1)
        gated_out = (gate_sig * attended_rows).astype(jnp.bfloat16)
        grad_gated = jnp.dot(cot_rows, out_weight.T, preferred_element_type=jnp.float32)
        grad_gate = grad_gated * attended_rows * gate_sig * (1.0 - gate_sig)
        attended_gradient = (
            (grad_gated * gate_sig)
            .astype(jnp.bfloat16)
            .reshape(sequence_length, local_heads, head_size)
        )
        probability_gradient = jnp.einsum(
            "fuc,suc->ufs", attended_gradient, value_rows, preferred_element_type=jnp.float32
        )
        value_gradient = jnp.einsum(
            "avj,vat->jat", attention_probs, attended_gradient, preferred_element_type=jnp.float32
        )
        grad_score = attention * (
            probability_gradient - jnp.sum(attention * probability_gradient, -1, keepdims=True)
        )
        score_gradient = grad_score.astype(jnp.bfloat16)
        query_gradient = (
            jnp.einsum(
                "vkq,qvy->kvy", score_gradient, key_matrix, preferred_element_type=jnp.float32
            )
            * inverse_square_root
        )
        key_gradient = (
            jnp.einsum(
                "avj,vat->jat", score_gradient, query_rows, preferred_element_type=jnp.float32
            )
            * inverse_square_root
        )
        grads = jnp.stack(
            [
                query_gradient.reshape(sequence_length, -1),
                key_gradient.reshape(sequence_length, -1),
                value_gradient.reshape(sequence_length, -1),
                grad_gate,
            ]
        ).astype(jnp.bfloat16)
        weight_sums = weight_sums + jnp.einsum(
            "nd,gne->gde", hidden, grads, preferred_element_type=jnp.float32
        )
        output_sums = output_sums + jnp.dot(
            gated_out.T, cot_rows, preferred_element_type=jnp.float32
        )
        return ((bias_sums + grad_score, weight_sums, output_sums), (gated_out, grads))

    start_sums = (
        jnp.zeros((local_heads, token_count, token_count), jnp.float32),
        jnp.zeros(attn_weight.shape, jnp.float32),
        jnp.zeros(out_weight.shape, jnp.float32),
    )
    final_sums, stacked = lax.scan(one_copy, start_sums, (tokens, cotangent, scales))
    bias_sums, weight_sums, output_sums = final_sums
    gated_all, grads_all = stacked
    token_share = token_count // lax.axis_size("col")
    attn_parts = jnp.einsum(
        "tnd,de->tne", gated_all, out_weight, preferred_element_type=jnp.float32
    )
    hidden_parts = jnp.einsum(
        "tgne,gde->tnd", grads_all, attn_weight, preferred_element_type=jnp.float32
    )
    attn_out, grad_hidden = (
        lax.psum_scatter(attn_parts, "col", scatter_dimension=1, tiled=True),
        lax.psum_scatter(hidden_parts, "col", scatter_dimension=1, tiled=True),
    )
    first_token = col_index * token_share
    token_mine = lax.dynamic_slice_in_dim(tokens, first_token, token_share, 1)
    cot_mine = lax.dynamic_slice_in_dim(cotangent, first_token, token_share, 1)
    scaled_mine = scales[:, None, None] * token_mine.astype(jnp.float32)
    denoised = (scaled_mine + attn_out).astype(jnp.bfloat16)
    grad_scaled = cot_mine.astype(jnp.float32) + norm_back(grad_hidden, scaled_mine, attn_gain)
    token_grad = (scales[:, None, None] * grad_scaled).astype(jnp.bfloat16)
    bias_rows_sum, out_grad, weight_grad = (
        lax.psum_scatter(bias_sums, ("group", "row"), scatter_dimension=1, tiled=True),
        lax.psum_scatter(output_sums, ("group", "row"), scatter_dimension=1, tiled=True),
        lax.psum_scatter(weight_sums, ("group", "row"), scatter_dimension=1, tiled=True),
    )
    bias_back = lax.all_to_all(bias_rows_sum, "col", split_axis=2, concat_axis=0, tiled=True)
    grad_bias = jnp.transpose(bias_back, (1, 2, 0)).reshape(-1, heads_all)
    grad_in = jnp.dot(
        grad_bias, bias_weight.astype(jnp.float32).T, precision=lax.Precision.HIGHEST
    ).reshape(rows_here, cols_here, channels)
    pair_grad = norm_back(grad_in, updated, bias_gain)
    weight_part = jnp.dot(
        flat_bias.astype(jnp.float32).T, grad_bias, precision=lax.Precision.HIGHEST
    )
    bias_weight_grad = lax.psum(weight_part, ("group", "row", "col"))
    return (
        updated.astype(jnp.bfloat16),
        pair_grad,
        bias_weight_grad,
        denoised,
        token_grad,
        weight_grad,
        out_grad,
    )


LANES = 128


def dot_nn(a, b, **kw):
    return lax.dot_general(a, b, (((1,), (0,)), ((), ())), preferred_element_type=jnp.float32, **kw)


def dot_nt(a, b, **kw):
    return lax.dot_general(a, b, (((1,), (1,)), ((), ())), preferred_element_type=jnp.float32, **kw)


def dot_tn(a, b, **kw):
    return lax.dot_general(a, b, (((0,), (0,)), ((), ())), preferred_element_type=jnp.float32, **kw)


def turn(values, groups, width):
    shift = (groups * width) % LANES
    return values if shift == 0 else pltpu.roll(values, shift, 1)


def merge(pieces, lane_group):
    merged = pieces[0]
    for g in range(1, len(pieces)):
        merged = jnp.where(lane_group == g, pieces[g], merged)
    return merged


def lane_groups(rows, width):
    return lax.broadcasted_iota(jnp.int32, (rows, LANES), 1) // width


def channel_order(channels, devices):
    r = lax.broadcasted_iota(jnp.int32, (channels, channels), 0)
    c = lax.broadcasted_iota(jnp.int32, (channels, channels), 1)
    return (r % devices) * (channels // devices) + r // devices == c


def whole(shape, dtype):
    return jax.ShapeDtypeStruct(shape, dtype)


def far(values):
    return pltpu.with_memory_space_constraint(values, pltpu.HBM)


def pair_in_kernel(pair_ref, mask_ref, gain_ref, proj_ref, out_ref, rows_ref):
    devices = out_ref.shape[0]
    rows, width = mask_ref.shape
    channels = pair_ref.shape[1]
    groups = LANES // width
    pair_in = (normalize(pair_ref[...].astype(jnp.float32)) * gain_ref[...]).astype(jnp.bfloat16)
    order = channel_order(channels, devices).astype(jnp.float32).astype(jnp.bfloat16)
    lanes = lane_groups(devices, width)
    mask = jnp.concatenate([mask_ref[...].astype(jnp.float32)] * groups, axis=1)
    for side in range(2):
        first = 2 * side * channels
        gate_t = dot_nt(order, proj_ref[:, first : first + channels]).astype(jnp.bfloat16)
        value_t = dot_nt(order, proj_ref[:, first + channels : first + 2 * channels]).astype(
            jnp.bfloat16
        )
        product = jax.nn.sigmoid(dot_nt(gate_t, pair_in)) * dot_nt(value_t, pair_in)
        for i in range(rows):
            q, s = divmod(i, groups)
            tile = merge(
                [
                    turn(
                        product[g * devices : (g + 1) * devices, q * LANES : (q + 1) * LANES],
                        g - s,
                        width,
                    )
                    for g in range(groups)
                ],
                lanes,
            )
            rows_ref[pl.ds(i, devices, stride=rows), :] = tile * mask[i : i + 1]
        out_ref[:, side] = rows_ref[...].astype(jnp.bfloat16).reshape(devices, rows, LANES)


def triangle_kernel(in_ref, out_ref, *, width):
    stripes, cols, _, rows, _ = in_ref.shape
    groups = LANES // width
    tokens = stripes * rows
    lanes = lane_groups(tokens, width)
    totals = [jnp.zeros((tokens, LANES), jnp.float32) for _ in range(groups)]
    for col in range(cols):
        left = in_ref[:, col, 0].reshape(tokens, LANES)
        right = in_ref[:, col, 1].reshape(tokens, LANES)
        for g in range(groups):
            totals[g] += dot_nt(jnp.where(lanes == g, left, jnp.zeros_like(left)), right)
    for col in range(cols):
        out_ref[:, col] = (
            merge([turn(totals[g], g - col, width) for g in range(groups)], lanes)
            .astype(jnp.bfloat16)
            .reshape(stripes, rows, LANES)
        )


def pair_out_kernel(
    here_ref,
    chain_ref,
    in_ref,
    pair_ref,
    chain_row_ref,
    in_gain_ref,
    gate_ref,
    out_gain_ref,
    out_weight_ref,
    bias_gain_ref,
    bias_weight_ref,
    chain_bias_ref,
    next_ref,
    updated_ref,
    bias_ref,
    rows_ref,
    *,
    width,
):
    devices, rows, _ = in_ref.shape
    stripes, cols = bias_ref.shape[:2]
    channels = pair_ref.shape[1]
    heads = bias_weight_ref.shape[0]
    groups = LANES // width

    def all_lanes(sums):
        total = sums
        for g in range(1, groups):
            total = total + turn(sums, g, width)
        return total

    triangle = in_ref[...].astype(jnp.float32)
    average = all_lanes(jnp.sum(triangle, 0)) * (1.0 / channels)
    centred = triangle - average
    inverse = lax.rsqrt(all_lanes(jnp.sum(centred * centred, 0)) * (1.0 / channels) + EPSILON)
    rows_ref[...] = (centred * inverse).reshape(devices * rows, LANES)
    lanes = lane_groups(devices, width)
    blocks = []
    for q in range(rows // groups):
        tiles = [
            rows_ref[pl.ds(q * groups + s, devices, stride=rows), :] for s in range(groups)
        ]
        blocks.append(
            jnp.concatenate(
                [
                    merge([turn(tiles[s], s - g, width) for s in range(groups)], lanes)
                    for g in range(groups)
                ],
                axis=0,
            )
        )
    normed_t = jnp.concatenate(blocks, axis=1)
    order = channel_order(channels, devices)
    gain_t = jnp.sum(jnp.where(order, out_gain_ref[...], 0.0), axis=1, keepdims=True)
    order_b = order.astype(jnp.float32).astype(jnp.bfloat16)
    weight = dot_nn(order_b, out_weight_ref[...]).astype(jnp.bfloat16)
    update = dot_tn((normed_t * gain_t).astype(jnp.bfloat16), weight)
    pair = pair_ref[...].astype(jnp.float32)
    pair_in = (normalize(pair) * in_gain_ref[...]).astype(jnp.bfloat16)
    updated = pair + jax.nn.sigmoid(dot_nn(pair_in, gate_ref[...])) * update
    updated_ref[...] = updated
    next_ref[...] = updated.astype(jnp.bfloat16)
    bias_in = (normalize(updated) * bias_gain_ref[...]).astype(jnp.bfloat16)
    unit = lax.broadcasted_iota(jnp.int32, (heads, heads), 0) == lax.broadcasted_iota(
        jnp.int32, (heads, heads), 1
    )
    chain_t = jnp.sum(jnp.where(unit, chain_bias_ref[...], 0.0), axis=1, keepdims=True)
    bias_t = dot_nt(bias_weight_ref[...], bias_in)
    lanes_h = lane_groups(heads, width)
    chain_row = jnp.broadcast_to(chain_row_ref[...], (heads, LANES))
    col_chain = merge(
        [
            pltpu.roll(chain_row, (g + cols - here_ref[1]) % cols * width, 1)
            for g in range(groups)
        ],
        lanes_h,
    )
    head_group = lax.broadcasted_iota(jnp.int32, (heads, LANES), 0) % groups
    spread = []
    for i in range(rows):
        q, s = divmod(i, groups)
        block = bias_t[:, q * LANES : (q + 1) * LANES]
        tile = jnp.zeros_like(block)
        for g in range(groups):
            tile = jnp.where(
                (lanes_h == g) & (head_group == g), turn(block, g - s, width), tile
            )
        row_chain = chain_ref[here_ref[0] * rows + i]
        extra = jnp.where((col_chain == row_chain) & (lanes_h == head_group), chain_t, 0.0)
        spread.append(tile + extra)
    spread = jnp.concatenate(spread, axis=0).astype(jnp.bfloat16)
    packed = dot_nn(head_gather(rows, cols, heads).astype(jnp.bfloat16), spread)
    packed = packed.astype(jnp.bfloat16).reshape(cols, rows, LANES)
    for stripe in range(stripes):
        bias_ref[stripe] = packed


def head_gather(rows, cols, heads):
    a = lax.broadcasted_iota(jnp.int32, (cols * rows, rows * heads), 0)
    b = lax.broadcasted_iota(jnp.int32, (cols * rows, rows * heads), 1)
    return ((a % rows == b // heads) & (a // rows == (b % heads) // (heads // cols))).astype(
        jnp.float32
    )


def token_in_kernel(
    scale_ref,
    tokens_ref,
    cot_ref,
    gain_ref,
    weight_ref,
    out_weight_ref,
    query_ref,
    key_ref,
    value_ref,
    gated_ref,
    sig_ref,
    grad_ref,
    score_ref,
    prob_ref,
    hidden_t_ref,
    cot_t_ref,
    hidden_ref,
    *,
    head_size,
):
    copies, length, _ = tokens_ref.shape
    inner = query_ref.shape[1]
    inverse_square_root = 1.0 / math.sqrt(head_size)
    for t in range(copies):
        part = slice(t * length, (t + 1) * length)
        scaled = scale_ref[t] * tokens_ref[t].astype(jnp.float32)
        hidden = normalize(scaled) * gain_ref[...]
        hidden_ref[part] = hidden.astype(jnp.bfloat16)
        hidden_t_ref[:, part] = hidden.T.astype(jnp.bfloat16)
        cot_t_ref[:, part] = cot_ref[t].astype(jnp.float32).T.astype(jnp.bfloat16)
    hidden = hidden_ref[...]
    query_ref[...] = dot_nt(hidden, weight_ref[0]).astype(jnp.bfloat16)
    key_ref[...] = dot_nt(hidden, weight_ref[1]).astype(jnp.bfloat16)
    value_ref[...] = dot_nt(hidden, weight_ref[2]).astype(jnp.bfloat16)
    sig = jax.nn.sigmoid(dot_nt(hidden, weight_ref[3]))
    sig_ref[...] = sig
    grad = dot_nt(cot_ref[...].reshape(copies * length, -1), out_weight_ref[...])
    grad_ref[...] = grad
    gated_ref[...] = (grad * sig).astype(jnp.bfloat16)
    head_of = lax.broadcasted_iota(jnp.int32, (length, inner), 1) // head_size
    for t in range(copies):
        part = slice(t * length, (t + 1) * length)
        query, key_rows, value, gated = (
            r[part] for r in (query_ref, key_ref, value_ref, gated_ref)
        )
        for h in range(score_ref.shape[1]):
            mine = head_of == h
            query_h = jnp.where(mine, query, jnp.zeros_like(query))
            gated_h = jnp.where(mine, gated, jnp.zeros_like(gated))
            score_ref[t, h] = dot_nt(query_h, key_rows) * inverse_square_root
            prob_ref[t, h] = dot_nt(gated_h, value)


def attention_kernel(
    here_ref,
    bias_ref,
    query_ref,
    key_ref,
    value_ref,
    gated_ref,
    sig_ref,
    grad_ref,
    score_ref,
    prob_ref,
    weight_ref,
    out_weight_ref,
    pair_ref,
    outs_ref,
    grads_ref,
    *refs,
    width,
    head_size,
):
    part_refs, (sums_ref, parts_ref) = refs[:-2], refs[-2:]
    stripes, cols, rows, _ = bias_ref.shape
    copies, heads, length, _ = score_ref.shape
    inner, hidden_width = out_weight_ref.shape
    share = length // cols
    lanes = lane_groups(length, width)
    head_of = lax.broadcasted_iota(jnp.int32, (length, inner), 1) // head_size
    inverse_square_root = 1.0 / math.sqrt(head_size)
    tiles = [
        bias_ref[:, col].astype(jnp.float32).reshape(length, LANES) for col in range(cols)
    ]
    bias = [
        merge([turn(tiles[col], col - h, width) for col in range(cols)], lanes)
        for h in range(heads)
    ]
    for t in range(copies):
        part = slice(t * length, (t + 1) * length)
        query, key_rows, value, gated = (
            r[part] for r in (query_ref, key_ref, value_ref, gated_ref)
        )
        attended = jnp.zeros((length, inner), jnp.float32)
        grad_query, grad_key, grad_value = attended, attended, attended
        for h in range(heads):
            mine = head_of == h
            query_h, key_h, value_h, gated_h = (
                jnp.where(mine, r, jnp.zeros_like(r)) for r in (query, key_rows, value, gated)
            )
            exponent = jnp.exp(score_ref[t, h] + bias[h])
            attention = exponent / jnp.sum(exponent, -1, keepdims=True)
            attention_b = attention.astype(jnp.bfloat16)
            grad_prob = prob_ref[t, h]
            grad_score = attention * (
                grad_prob - jnp.sum(attention * grad_prob, -1, keepdims=True)
            )
            sums_ref[h] = grad_score if t == 0 else sums_ref[h] + grad_score
            score_b = grad_score.astype(jnp.bfloat16)
            attended += dot_nn(attention_b, value_h)
            grad_query += dot_nn(score_b, key_h)
            grad_key += dot_tn(score_b, query_h)
            grad_value += dot_tn(attention_b, gated_h)
        sig = sig_ref[part]
        gated_out = (sig * attended).astype(jnp.bfloat16)
        grads = [
            (grad_query * inverse_square_root).astype(jnp.bfloat16),
            (grad_key * inverse_square_root).astype(jnp.bfloat16),
            grad_value.astype(jnp.bfloat16),
            (grad_ref[part] * attended * sig * (1.0 - sig)).astype(jnp.bfloat16),
        ]
        outs_ref[part] = gated_out
        for g in range(4):
            grads_ref[g, part] = grads[g]
        out_part = dot_nn(gated_out, out_weight_ref[...])
        in_part = dot_nn(grads[0], weight_ref[0])
        for g in range(1, 4):
            in_part += dot_nn(grads[g], weight_ref[g])
        parts_ref[:, 0, t] = out_part.astype(jnp.bfloat16).reshape(cols, share, hidden_width)
        parts_ref[:, 1, t] = in_part.astype(jnp.bfloat16).reshape(cols, share, hidden_width)
    for k in range(cols):
        part_refs[k][...] = parts_ref[(here_ref[1] + k) % cols]
    for col in range(cols):
        pair_ref[:, col] = (
            merge([turn(sums_ref[h], h - col, width) for h in range(heads)], lanes)
            .astype(jnp.bfloat16)
            .reshape(stripes, rows, LANES)
        )


def weight_in_kernel(
    here_ref, hidden_t_ref, cot_t_ref, grads_ref, outs_ref, keep_ref, send_ref, wire_ref
):
    hidden_t = hidden_t_ref[...]
    chips, _, block, _ = wire_ref.shape

    def put(values, first, last):
        wire_ref[:, :, :, first * LANES : last * LANES] = values.astype(jnp.bfloat16).reshape(
            chips, 2, block, -1
        )

    weights = [dot_nn(hidden_t, grads_ref[g]) for g in range(4)]
    weights.append(dot_nn(cot_t_ref[...], outs_ref[...]))
    for g in range(5):
        put(weights[g][:, :LANES], g, g + 1)
    tails = [w[:, LANES:] for w in weights]
    tails.append(jnp.zeros_like(tails[0]))
    for g in range(3):
        put(jnp.concatenate(tails[2 * g : 2 * g + 2], axis=1), 5 + g, 6 + g)
    core = here_ref[0] % 2
    keep_ref[...] = wire_ref[:, core]
    send_ref[...] = wire_ref[:, 1 - core]


def weight_add_kernel(here_ref, keep_ref, got_ref, *refs):
    out_refs, sum_ref = refs[:-1], refs[-1]
    sum_ref[...] = (
        keep_ref[...].astype(jnp.float32) + got_ref[...].astype(jnp.float32)
    ).astype(jnp.bfloat16)
    chip = here_ref[0] // 2
    for k in range(len(out_refs)):
        out_refs[k][...] = sum_ref[chip ^ k]


def pair_back_kernel(
    in_ref, updated_ref, gain_ref, bias_weight_ref, grad_ref, weight_ref, *, width
):
    _, cols, rows, _ = in_ref.shape
    heads = bias_weight_ref.shape[0]
    groups = LANES // width
    total = jnp.sum(in_ref[...].astype(jnp.float32), 0).reshape(cols * rows, LANES)
    spread = dot_tn(head_gather(rows, cols, heads), total, precision=lax.Precision.HIGHEST)
    lanes = lane_groups(heads, width)
    head_group = lax.broadcasted_iota(jnp.int32, (heads, LANES), 0) % groups
    blocks = []
    for q in range(rows // groups):
        tiles = []
        for s in range(groups):
            i = q * groups + s
            tile = spread[i * heads : (i + 1) * heads]
            turned = tile
            for g in range(groups):
                turned = jnp.where(head_group == g, turn(tile, s - g, width), turned)
            tiles.append(turned)
        blocks.append(merge(tiles, lanes))
    grad_t = jnp.concatenate(blocks, axis=1)
    updated = updated_ref[...]
    gain = gain_ref[...]
    grad_in = lax.dot_general(
        grad_t,
        bias_weight_ref[...].astype(jnp.float32),
        (((0,), (0,)), ((), ())),
        precision=lax.Precision.HIGHEST,
        preferred_element_type=jnp.float32,
    )
    grad_ref[...] = norm_back(grad_in, updated, gain)
    bias_in = (normalize(updated) * gain).astype(jnp.bfloat16).astype(jnp.float32)
    weight = dot_nn(grad_t, bias_in, precision=lax.Precision.HIGHEST).astype(jnp.bfloat16)
    for device in range(weight_ref.shape[0]):
        weight_ref[device] = weight


def token_out_kernel(here_ref, scale_ref, tokens_ref, cot_ref, gain_ref, *refs):
    part_refs, (out_ref, grad_ref) = refs[:-2], refs[-2:]
    for t in range(out_ref.shape[0]):
        sums = part_refs[0][:, t].astype(jnp.float32)
        for r in part_refs[1:]:
            sums = sums + r[:, t].astype(jnp.float32)
        scale = scale_ref[t]
        scaled = scale * tokens_ref[t].astype(jnp.float32)
        out_ref[t] = (scaled + sums[0]).astype(jnp.bfloat16)
        grad = cot_ref[t].astype(jnp.float32) + norm_back(sums[1], scaled, gain_ref[...])
        grad_ref[t] = (scale * grad).astype(jnp.bfloat16)


def weight_out_kernel(*refs):
    in_refs, (grad_ref, out_ref) = refs[:-2], refs[-2:]
    total = in_refs[0][...].astype(jnp.float32)
    for r in in_refs[1:]:
        total = total + r[...].astype(jnp.float32)
    half = LANES // 2
    for g in range(4):
        grad_ref[g, :, :LANES] = total[:, g * LANES : (g + 1) * LANES]
        first = (5 + g // 2) * LANES + (g % 2) * half
        grad_ref[g, :, LANES:] = total[:, first : first + half]
    rows = jnp.concatenate(
        [total[:, 4 * LANES : 5 * LANES], total[:, 7 * LANES : 8 * LANES]], axis=1
    )
    out_ref[...] = rows.T[: out_ref.shape[0]]


def fits(pair_repr, token_count, heads_all, inner, hidden_width, stripes, cols):
    rows, width, channels = pair_repr.shape
    groups = LANES // width if LANES % width == 0 else 0
    return (
        groups > 0
        and token_count == LANES
        and channels == LANES
        and channels == stripes * cols * groups
        and cols == groups
        and heads_all == cols * groups
        and rows % 16 == 0
        and stripes * rows == token_count
        and stripes % 2 == 0
        and stripes & (stripes - 1) == 0
        and inner == LANES + LANES // 2
        and hidden_width % (16 * stripes) == 0
    )


def shards(
    pair_repr,
    pair_mask,
    chain_id,
    tri_in_gain,
    tri_proj,
    tri_gate,
    tri_out_gain,
    tri_out,
    bias_gain,
    bias_weight,
    chain_bias,
    tokens,
    noise_level,
    attn_gain,
    attn_weight,
    out_weight,
    cotangent,
):
    stripe_axes = ("group", "row")
    all_axes = ("group", "row", "col")
    stripes = lax.axis_size(stripe_axes)
    cols = lax.axis_size("col")
    rows, width, channels = pair_repr.shape
    heads_all = bias_weight.shape[1]
    copies, length, hidden_width = tokens.shape
    inner = attn_weight.shape[2]
    if not fits(pair_repr, length, heads_all, inner, hidden_width, stripes, cols):
        return general_shards(
            pair_repr,
            pair_mask,
            chain_id,
            tri_in_gain,
            tri_proj,
            tri_gate,
            tri_out_gain,
            tri_out,
            bias_gain,
            bias_weight,
            chain_bias,
            tokens,
            noise_level,
            attn_gain,
            attn_weight,
            out_weight,
            cotangent,
        )
    head_size = hidden_width // heads_all
    devices = stripes * cols
    pairs = rows * width
    bf16, f32 = jnp.bfloat16, jnp.float32
    vmem = pl.BlockSpec(memory_space=pltpu.VMEM)
    smem = pl.BlockSpec(memory_space=pltpu.SMEM)
    row_index = lax.axis_index(stripe_axes)
    col_index = lax.axis_index("col")
    here = jnp.stack([row_index, col_index]).astype(jnp.int32)
    pair_flat = pair_repr.reshape(pairs, channels)
    scales = noise_scale(noise_level)
    weight_t = jnp.swapaxes(attn_weight, 1, 2)
    bias_weight_t = bias_weight.T

    def call(kernel, mib, out_shape, n_smem, n_vmem, scratch=(), **options):
        many = isinstance(out_shape, tuple)
        return pl.pallas_call(
            functools.partial(kernel, **options),
            out_shape=out_shape,
            in_specs=[smem] * n_smem + [vmem] * n_vmem,
            out_specs=(vmem,) * len(out_shape) if many else vmem,
            scratch_shapes=list(scratch),
            compiler_params=pltpu.CompilerParams(vmem_limit_bytes=mib << 20),
        )

    def exchange(values, axes):
        return lax.all_to_all(values, axes, 0, 0, tiled=True)

    def shift(values, k):
        return lax.ppermute(values, "col", [(i, (i + k) % cols) for i in range(cols)])

    projected = call(
        pair_in_kernel,
        8,
        whole((devices, 2, rows, LANES), bf16),
        0,
        4,
        [pltpu.VMEM((devices * rows, LANES), f32)],
    )(far(pair_flat), far(pair_mask), far(tri_in_gain[None]), far(tri_proj))
    sides = exchange(projected.reshape(devices, 2 * rows, LANES), all_axes)
    tall = copies * length
    local = heads_all // cols
    query, key_rows, value, gated, gate_sig, grad_gated, scores, probs, hidden_t, cot_t = call(
        token_in_kernel,
        16,
        (
            *[pltpu.HBM((tall, inner), bf16)] * 4,
            *[pltpu.HBM((tall, inner), f32)] * 2,
            *[pltpu.HBM((copies, local, length, length), f32)] * 2,
            *[pltpu.HBM((hidden_width, tall), bf16)] * 2,
        ),
        1,
        5,
        [pltpu.VMEM((tall, hidden_width), bf16)],
        head_size=head_size,
    )(
        scales, *map(far, (tokens, cotangent, attn_gain[None], weight_t, out_weight))
    )
    triangle = call(
        triangle_kernel, 8, whole((stripes, cols, rows, LANES), bf16), 0, 1, width=width
    )(sides.reshape(stripes, cols, 2, rows, LANES))
    triangle = exchange(triangle.reshape(devices, rows, LANES), all_axes)
    pair_next, updated, bias_tile = call(
        pair_out_kernel,
        8,
        (
            pltpu.HBM((pairs, channels), bf16),
            pltpu.HBM((pairs, channels), f32),
            whole((stripes, cols, rows, LANES), bf16),
        ),
        2,
        10,
        [pltpu.VMEM((devices * rows, LANES), f32)],
        width=width,
    )(
        here,
        chain_id,
        triangle,
        *map(
            far,
            (
                pair_flat,
                chain_id[None],
                tri_in_gain[None],
                tri_gate,
                tri_out_gain[None],
                tri_out,
                bias_gain[None],
                bias_weight_t,
                chain_bias[None],
            ),
        ),
    )
    head_bias = exchange(bias_tile.reshape(devices, rows, LANES), all_axes)
    part = pltpu.HBM((2, copies, length // cols, hidden_width), bf16)
    bias_sums, outs, grads, *parts = call(
        attention_kernel,
        20,
        (
            whole((stripes, cols, rows, LANES), bf16),
            pltpu.HBM((tall, inner), bf16),
            pltpu.HBM((4, tall, inner), bf16),
            *[part] * cols,
        ),
        1,
        11,
        [
            pltpu.VMEM((local, length, length), f32),
            pltpu.VMEM((cols, 2, copies, length // cols, hidden_width), bf16),
        ],
        width=width,
        head_size=head_size,
    )(
        here,
        head_bias.reshape(stripes, cols, rows, LANES),
        *map(
            far,
            (
                query,
                key_rows,
                value,
                gated,
                gate_sig,
                grad_gated,
                scores,
                probs,
                weight_t,
                out_weight,
            ),
        ),
    )
    bias_back = exchange(bias_sums.reshape(devices, rows, LANES), all_axes)
    received = [parts[0]] + [shift(parts[k], k) for k in range(1, cols)]
    chips = stripes // 2
    block = hidden_width // stripes
    keep, give = call(
        weight_in_kernel,
        16,
        (pltpu.HBM((chips, block, 8 * LANES), bf16),) * 2,
        1,
        4,
        [pltpu.VMEM((chips, 2, block, 8 * LANES), bf16)],
    )(here, *map(far, (hidden_t, cot_t, grads, outs)))
    got = lax.ppermute(give, stripe_axes, [(i, i ^ 1) for i in range(stripes)])
    mine, *give = call(
        weight_add_kernel,
        12,
        (pltpu.HBM((block, 8 * LANES), bf16),) * chips,
        1,
        2,
        [pltpu.VMEM((chips, block, 8 * LANES), bf16)],
    )(here, far(keep), got)
    wires = [mine]
    for k in range(1, chips):
        wires.append(
            lax.ppermute(
                give[k - 1], stripe_axes, [(i, i ^ (2 * k)) for i in range(stripes)]
            )
        )
    pair_grad, weight_part = call(
        pair_back_kernel,
        8,
        (whole((pairs, channels), f32), whole((devices, heads_all, channels), bf16)),
        0,
        4,
        width=width,
    )(
        bias_back.reshape(stripes, cols, rows, LANES),
        *map(far, (updated, bias_gain[None], bias_weight_t)),
    )
    weight_part = exchange(weight_part, all_axes)
    bias_weight_grad = jnp.sum(weight_part.astype(f32), 0).T
    weight_grad, out_grad = call(
        weight_out_kernel,
        16,
        (
            whole((4, hidden_width // stripes, inner), f32),
            whole((inner, hidden_width // stripes), f32),
        ),
        0,
        chips,
    )(far(wires[0]), *wires[1:])
    share = length // cols
    mine = pl.BlockSpec((copies, share, hidden_width), lambda i, here: (0, here[1], 0))
    fixed = lambda shape: pl.BlockSpec(shape, lambda i, here: (0,) * len(shape))
    denoised, token_grad = pl.pallas_call(
        token_out_kernel,
        grid_spec=pltpu.PrefetchScalarGridSpec(
            num_scalar_prefetch=1,
            grid=(1,),
            in_specs=[smem, mine, mine, fixed((1, hidden_width))] + [fixed((2, copies, share, hidden_width))] * cols,
            out_specs=[fixed((copies, share, hidden_width))] * 2,
        ),
        out_shape=(whole((copies, share, hidden_width), bf16),) * 2,
        compiler_params=pltpu.CompilerParams(vmem_limit_bytes=16 << 20),
        name="token_out",
    )(here, scales, tokens, cotangent, attn_gain[None], *received)
    return (
        pair_next.reshape(rows, width, channels),
        pair_grad.reshape(rows, width, channels),
        bias_weight_grad,
        denoised,
        token_grad,
        weight_grad,
        out_grad,
    )


def solution(mesh):
    return jax.shard_map(
        shards,
        mesh=mesh,
        in_specs=(
            P(("group", "row"), "col", None),
            P(("group", "row"), "col"),
            P(),
            P(),
            P(),
            P(),
            P(),
            P(),
            P(),
            P(),
            P(),
            P(("group", "row"), None, None),
            P(("group", "row")),
            P(),
            P(None, None, "col"),
            P("col", None),
            P(("group", "row"), None, None),
        ),
        out_specs=(
            P(("group", "row"), "col", None),
            P(("group", "row"), "col", None),
            P(),
            P(("group", "row"), "col", None),
            P(("group", "row"), "col", None),
            P(None, ("group", "row"), "col"),
            P("col", ("group", "row")),
        ),
        check_vma=False,
    )
```

```python
import functools
import math

import jax
import jax.numpy as jnp
from jax import lax
from jax.experimental import pallas as pl
from jax.experimental.pallas import tpu as pltpu
from jax.sharding import PartitionSpec as P


LEVELS = 200


EPSILON = 1e-05
SIGMA_LOW = 0.1
SIGMA_SPAN = 100.0


def normalize(values):
    average = jnp.mean(values, -1, keepdims=True)
    centred = values - average
    return centred * lax.rsqrt(jnp.mean(centred * centred, -1, keepdims=True) + EPSILON)


def norm_back(gradient, values, norm_gain):
    average = jnp.mean(values, -1, keepdims=True)
    centred = values - average
    inverse = lax.rsqrt(jnp.mean(centred * centred, -1, keepdims=True) + EPSILON)
    normed = centred * inverse
    weighted = gradient * norm_gain
    return inverse * (
        weighted
        - jnp.mean(weighted, -1, keepdims=True)
        - normed * jnp.mean(weighted * normed, -1, keepdims=True)
    )


def noise_scale(levels):
    sigma_vals = SIGMA_LOW * SIGMA_SPAN ** (levels.astype(jnp.float32) / (LEVELS - 1))
    return lax.rsqrt(1.0 + sigma_vals * sigma_vals)


def general_shards(
    pair_repr,
    pair_mask,
    chain_id,
    tri_in_gain,
    tri_proj,
    tri_gate,
    tri_out_gain,
    tri_out,
    bias_gain,
    bias_weight,
    chain_bias,
    tokens,
    noise_level,
    attn_gain,
    attn_weight,
    out_weight,
    cotangent,
):
    rows_here = pair_repr.shape[0]
    cols_here = pair_repr.shape[1]
    channels = pair_repr.shape[2]
    token_count = chain_id.shape[0]
    heads_all = bias_weight.shape[1]
    hidden_width = attn_gain.shape[0]
    head_size = hidden_width // heads_all
    inverse_square_root = 1.0 / math.sqrt(head_size)
    row_index = lax.axis_index(("group", "row"))
    col_index = lax.axis_index("col")
    pair_tile = pair_repr.astype(jnp.float32)
    pair_in = (normalize(pair_tile) * tri_in_gain).astype(jnp.bfloat16)
    flat_in = pair_in.reshape(-1, channels)
    projected = jnp.dot(flat_in, tri_proj, preferred_element_type=jnp.float32).reshape(
        rows_here, cols_here, 4, channels
    )
    mask_tile = pair_mask.astype(jnp.float32)[:, :, None]
    left_proj = (jax.nn.sigmoid(projected[:, :, 0]) * projected[:, :, 1] * mask_tile).astype(
        jnp.bfloat16
    )
    right_proj = (jax.nn.sigmoid(projected[:, :, 2]) * projected[:, :, 3] * mask_tile).astype(
        jnp.bfloat16
    )
    gate_act = jax.nn.sigmoid(
        jnp.dot(flat_in, tri_gate, preferred_element_type=jnp.float32)
    ).reshape(rows_here, cols_here, channels)
    left_major = jnp.transpose(left_proj, (2, 0, 1))
    right_major = jnp.transpose(right_proj, (2, 0, 1))
    partial_rows = jnp.einsum(
        "cjk,cik->cji",
        lax.all_gather(right_major, ("group", "row"), axis=1, tiled=True),
        left_major,
        preferred_element_type=jnp.float32,
    )
    summed = lax.psum_scatter(partial_rows, "col", scatter_dimension=1, tiled=True)
    triangle = jnp.transpose(summed, (2, 1, 0))
    tri_normed = (normalize(triangle) * tri_out_gain).astype(jnp.bfloat16)
    update = jnp.dot(
        tri_normed.reshape(-1, channels), tri_out, preferred_element_type=jnp.float32
    ).reshape(rows_here, cols_here, channels)
    updated = pair_tile + gate_act * update
    bias_in = (normalize(updated) * bias_gain).astype(jnp.bfloat16)
    flat_bias = bias_in.reshape(-1, channels)
    bias_tile = jnp.dot(flat_bias, bias_weight, preferred_element_type=jnp.float32).reshape(
        rows_here, cols_here, heads_all
    )
    row_chain = lax.dynamic_slice_in_dim(chain_id, row_index * rows_here, rows_here)
    col_chain = lax.dynamic_slice_in_dim(chain_id, col_index * cols_here, cols_here)
    same_chain = (row_chain[:, None] == col_chain[None, :]).astype(jnp.float32)
    bias_tile = bias_tile + same_chain[:, :, None] * chain_bias
    bias_major = jnp.transpose(bias_tile.astype(jnp.bfloat16), (2, 0, 1))
    head_rows = lax.all_to_all(bias_major, "col", split_axis=0, concat_axis=2, tiled=True)
    per_head_bias = lax.all_gather(head_rows, ("group", "row"), axis=1, tiled=True).astype(
        jnp.float32
    )
    local_heads = per_head_bias.shape[0]
    scales = noise_scale(noise_level)

    def one_copy(carried, inputs):
        bias_sums, weight_sums, output_sums = carried
        token_rows, cot_rows, scaling = inputs
        sequence_length = token_rows.shape[0]
        scaled = scaling * token_rows.astype(jnp.float32)
        hidden = (normalize(scaled) * attn_gain).astype(jnp.bfloat16)
        projections = jnp.einsum(
            "nd,gde->gne", hidden, attn_weight, preferred_element_type=jnp.float32
        )
        query_rows = (
            projections[0].astype(jnp.bfloat16).reshape(sequence_length, local_heads, head_size)
        )
        key_matrix = (
            projections[1].astype(jnp.bfloat16).reshape(sequence_length, local_heads, head_size)
        )
        value_rows = (
            projections[2].astype(jnp.bfloat16).reshape(sequence_length, local_heads, head_size)
        )
        gate_sig = jax.nn.sigmoid(projections[3])
        logit_scores = (
            jnp.einsum("fuc,suc->ufs", query_rows, key_matrix, preferred_element_type=jnp.float32)
            * inverse_square_root
            + per_head_bias
        )
        exponent = jnp.exp(logit_scores)
        attention = exponent / jnp.sum(exponent, -1, keepdims=True)
        attention_probs = attention.astype(jnp.bfloat16)
        attended_rows = jnp.einsum(
            "vkq,qvy->kvy", attention_probs, value_rows, preferred_element_type=jnp.float32
        ).reshape(sequence_length, -1)
        gated_out = (gate_sig * attended_rows).astype(jnp.bfloat16)
        grad_gated = jnp.dot(cot_rows, out_weight.T, preferred_element_type=jnp.float32)
        grad_gate = grad_gated * attended_rows * gate_sig * (1.0 - gate_sig)
        attended_gradient = (
            (grad_gated * gate_sig)
            .astype(jnp.bfloat16)
            .reshape(sequence_length, local_heads, head_size)
        )
        probability_gradient = jnp.einsum(
            "fuc,suc->ufs", attended_gradient, value_rows, preferred_element_type=jnp.float32
        )
        value_gradient = jnp.einsum(
            "avj,vat->jat", attention_probs, attended_gradient, preferred_element_type=jnp.float32
        )
        grad_score = attention * (
            probability_gradient - jnp.sum(attention * probability_gradient, -1, keepdims=True)
        )
        score_gradient = grad_score.astype(jnp.bfloat16)
        query_gradient = (
            jnp.einsum(
                "vkq,qvy->kvy", score_gradient, key_matrix, preferred_element_type=jnp.float32
            )
            * inverse_square_root
        )
        key_gradient = (
            jnp.einsum(
                "avj,vat->jat", score_gradient, query_rows, preferred_element_type=jnp.float32
            )
            * inverse_square_root
        )
        grads = jnp.stack(
            [
                query_gradient.reshape(sequence_length, -1),
                key_gradient.reshape(sequence_length, -1),
                value_gradient.reshape(sequence_length, -1),
                grad_gate,
            ]
        ).astype(jnp.bfloat16)
        weight_sums = weight_sums + jnp.einsum(
            "nd,gne->gde", hidden, grads, preferred_element_type=jnp.float32
        )
        output_sums = output_sums + jnp.dot(
            gated_out.T, cot_rows, preferred_element_type=jnp.float32
        )
        return ((bias_sums + grad_score, weight_sums, output_sums), (gated_out, grads))

    start_sums = (
        jnp.zeros((local_heads, token_count, token_count), jnp.float32),
        jnp.zeros(attn_weight.shape, jnp.float32),
        jnp.zeros(out_weight.shape, jnp.float32),
    )
    final_sums, stacked = lax.scan(one_copy, start_sums, (tokens, cotangent, scales))
    bias_sums, weight_sums, output_sums = final_sums
    gated_all, grads_all = stacked
    token_share = token_count // lax.axis_size("col")
    attn_parts = jnp.einsum(
        "tnd,de->tne", gated_all, out_weight, preferred_element_type=jnp.float32
    )
    hidden_parts = jnp.einsum(
        "tgne,gde->tnd", grads_all, attn_weight, preferred_element_type=jnp.float32
    )
    attn_out, grad_hidden = (
        lax.psum_scatter(attn_parts, "col", scatter_dimension=1, tiled=True),
        lax.psum_scatter(hidden_parts, "col", scatter_dimension=1, tiled=True),
    )
    first_token = col_index * token_share
    token_mine = lax.dynamic_slice_in_dim(tokens, first_token, token_share, 1)
    cot_mine = lax.dynamic_slice_in_dim(cotangent, first_token, token_share, 1)
    scaled_mine = scales[:, None, None] * token_mine.astype(jnp.float32)
    denoised = (scaled_mine + attn_out).astype(jnp.bfloat16)
    grad_scaled = cot_mine.astype(jnp.float32) + norm_back(grad_hidden, scaled_mine, attn_gain)
    token_grad = (scales[:, None, None] * grad_scaled).astype(jnp.bfloat16)
    bias_rows_sum, out_grad, weight_grad = (
        lax.psum_scatter(bias_sums, ("group", "row"), scatter_dimension=1, tiled=True),
        lax.psum_scatter(output_sums, ("group", "row"), scatter_dimension=1, tiled=True),
        lax.psum_scatter(weight_sums, ("group", "row"), scatter_dimension=1, tiled=True),
    )
    bias_back = lax.all_to_all(bias_rows_sum, "col", split_axis=2, concat_axis=0, tiled=True)
    grad_bias = jnp.transpose(bias_back, (1, 2, 0)).reshape(-1, heads_all)
    grad_in = jnp.dot(
        grad_bias, bias_weight.astype(jnp.float32).T, precision=lax.Precision.HIGHEST
    ).reshape(rows_here, cols_here, channels)
    pair_grad = norm_back(grad_in, updated, bias_gain)
    weight_part = jnp.dot(
        flat_bias.astype(jnp.float32).T, grad_bias, precision=lax.Precision.HIGHEST
    )
    bias_weight_grad = lax.psum(weight_part, ("group", "row", "col"))
    return (
        updated.astype(jnp.bfloat16),
        pair_grad,
        bias_weight_grad,
        denoised,
        token_grad,
        weight_grad,
        out_grad,
    )


LANES = 128


def dot_nn(a, b, **kw):
    return lax.dot_general(a, b, (((1,), (0,)), ((), ())), preferred_element_type=jnp.float32, **kw)


def dot_nt(a, b, **kw):
    return lax.dot_general(a, b, (((1,), (1,)), ((), ())), preferred_element_type=jnp.float32, **kw)


def dot_tn(a, b, **kw):
    return lax.dot_general(a, b, (((0,), (0,)), ((), ())), preferred_element_type=jnp.float32, **kw)


def turn(values, groups, width):
    shift = (groups * width) % LANES
    return values if shift == 0 else pltpu.roll(values, shift, 1)


def merge(pieces, lane_group):
    merged = pieces[0]
    for g in range(1, len(pieces)):
        merged = jnp.where(lane_group == g, pieces[g], merged)
    return merged


def lane_groups(rows, width):
    return lax.broadcasted_iota(jnp.int32, (rows, LANES), 1) // width


def channel_order(channels, devices):
    r = lax.broadcasted_iota(jnp.int32, (channels, channels), 0)
    c = lax.broadcasted_iota(jnp.int32, (channels, channels), 1)
    return (r % devices) * (channels // devices) + r // devices == c


def whole(shape, dtype):
    return jax.ShapeDtypeStruct(shape, dtype)


def far(values):
    return pltpu.with_memory_space_constraint(values, pltpu.HBM)


def near(values):
    return pltpu.with_memory_space_constraint(values, pltpu.VMEM)


def pair_in_kernel(pair_ref, mask_ref, gain_ref, proj_ref, out_ref, rows_ref):
    devices = out_ref.shape[0]
    rows, width = mask_ref.shape
    channels = pair_ref.shape[1]
    groups = LANES // width
    pair_in = (normalize(pair_ref[...].astype(jnp.float32)) * gain_ref[...]).astype(jnp.bfloat16)
    order = channel_order(channels, devices).astype(jnp.float32).astype(jnp.bfloat16)
    lanes = lane_groups(devices, width)
    mask = jnp.concatenate([mask_ref[...].astype(jnp.float32)] * groups, axis=1)
    for side in range(2):
        first = 2 * side * channels
        gate_t = dot_nt(order, proj_ref[:, first : first + channels]).astype(jnp.bfloat16)
        value_t = dot_nt(order, proj_ref[:, first + channels : first + 2 * channels]).astype(
            jnp.bfloat16
        )
        product = jax.nn.sigmoid(dot_nt(gate_t, pair_in)) * dot_nt(value_t, pair_in)
        for i in range(rows):
            q, s = divmod(i, groups)
            tile = merge(
                [
                    turn(
                        product[g * devices : (g + 1) * devices, q * LANES : (q + 1) * LANES],
                        g - s,
                        width,
                    )
                    for g in range(groups)
                ],
                lanes,
            )
            rows_ref[pl.ds(i, devices, stride=rows), :] = tile * mask[i : i + 1]
        out_ref[:, side] = rows_ref[...].astype(jnp.bfloat16).reshape(devices, rows, LANES)


def triangle_kernel(in_ref, out_ref, *, width):
    stripes, cols, _, rows, _ = in_ref.shape
    groups = LANES // width
    tokens = stripes * rows
    lanes = lane_groups(tokens, width)
    totals = [jnp.zeros((tokens, LANES), jnp.float32) for _ in range(groups)]
    for col in range(cols):
        left = in_ref[:, col, 0].reshape(tokens, LANES)
        right = in_ref[:, col, 1].reshape(tokens, LANES)
        for g in range(groups):
            totals[g] += dot_nt(jnp.where(lanes == g, left, jnp.zeros_like(left)), right)
    for col in range(cols):
        out_ref[:, col] = (
            merge([turn(totals[g], g - col, width) for g in range(groups)], lanes)
            .astype(jnp.bfloat16)
            .reshape(stripes, rows, LANES)
        )


def pair_out_kernel(
    here_ref,
    chain_ref,
    in_ref,
    pair_ref,
    chain_row_ref,
    in_gain_ref,
    gate_ref,
    out_gain_ref,
    out_weight_ref,
    bias_gain_ref,
    bias_weight_ref,
    chain_bias_ref,
    next_ref,
    updated_ref,
    bias_ref,
    rows_ref,
    *,
    width,
):
    devices, rows, _ = in_ref.shape
    stripes, cols = bias_ref.shape[:2]
    channels = pair_ref.shape[1]
    heads = bias_weight_ref.shape[0]
    groups = LANES // width

    def all_lanes(sums):
        total = sums
        for g in range(1, groups):
            total = total + turn(sums, g, width)
        return total

    triangle = in_ref[...].astype(jnp.float32)
    average = all_lanes(jnp.sum(triangle, 0)) * (1.0 / channels)
    centred = triangle - average
    inverse = lax.rsqrt(all_lanes(jnp.sum(centred * centred, 0)) * (1.0 / channels) + EPSILON)
    rows_ref[...] = (centred * inverse).reshape(devices * rows, LANES)
    lanes = lane_groups(devices, width)
    blocks = []
    for q in range(rows // groups):
        tiles = [
            rows_ref[pl.ds(q * groups + s, devices, stride=rows), :] for s in range(groups)
        ]
        blocks.append(
            jnp.concatenate(
                [
                    merge([turn(tiles[s], s - g, width) for s in range(groups)], lanes)
                    for g in range(groups)
                ],
                axis=0,
            )
        )
    normed_t = jnp.concatenate(blocks, axis=1)
    order = channel_order(channels, devices)
    gain_t = jnp.sum(jnp.where(order, out_gain_ref[...], 0.0), axis=1, keepdims=True)
    order_b = order.astype(jnp.float32).astype(jnp.bfloat16)
    weight = dot_nn(order_b, out_weight_ref[...]).astype(jnp.bfloat16)
    update = dot_tn((normed_t * gain_t).astype(jnp.bfloat16), weight)
    pair = pair_ref[...].astype(jnp.float32)
    pair_in = (normalize(pair) * in_gain_ref[...]).astype(jnp.bfloat16)
    updated = pair + jax.nn.sigmoid(dot_nn(pair_in, gate_ref[...])) * update
    updated_ref[...] = updated
    next_ref[...] = updated.astype(jnp.bfloat16)
    bias_in = (normalize(updated) * bias_gain_ref[...]).astype(jnp.bfloat16)
    unit = lax.broadcasted_iota(jnp.int32, (heads, heads), 0) == lax.broadcasted_iota(
        jnp.int32, (heads, heads), 1
    )
    chain_t = jnp.sum(jnp.where(unit, chain_bias_ref[...], 0.0), axis=1, keepdims=True)
    bias_t = dot_nt(bias_weight_ref[...], bias_in)
    lanes_h = lane_groups(heads, width)
    chain_row = jnp.broadcast_to(chain_row_ref[...], (heads, LANES))
    col_chain = merge(
        [
            pltpu.roll(chain_row, (g + cols - here_ref[1]) % cols * width, 1)
            for g in range(groups)
        ],
        lanes_h,
    )
    head_group = lax.broadcasted_iota(jnp.int32, (heads, LANES), 0) % groups
    spread = []
    for i in range(rows):
        q, s = divmod(i, groups)
        block = bias_t[:, q * LANES : (q + 1) * LANES]
        tile = jnp.zeros_like(block)
        for g in range(groups):
            tile = jnp.where(
                (lanes_h == g) & (head_group == g), turn(block, g - s, width), tile
            )
        row_chain = chain_ref[here_ref[0] * rows + i]
        extra = jnp.where((col_chain == row_chain) & (lanes_h == head_group), chain_t, 0.0)
        spread.append(tile + extra)
    spread = jnp.concatenate(spread, axis=0).astype(jnp.bfloat16)
    packed = dot_nn(head_gather(rows, cols, heads).astype(jnp.bfloat16), spread)
    packed = packed.astype(jnp.bfloat16).reshape(cols, rows, LANES)
    for stripe in range(stripes):
        bias_ref[stripe] = packed


def head_gather(rows, cols, heads):
    a = lax.broadcasted_iota(jnp.int32, (cols * rows, rows * heads), 0)
    b = lax.broadcasted_iota(jnp.int32, (cols * rows, rows * heads), 1)
    return ((a % rows == b // heads) & (a // rows == (b % heads) // (heads // cols))).astype(
        jnp.float32
    )


def token_in_kernel(
    scale_ref,
    tokens_ref,
    cot_ref,
    gain_ref,
    weight_ref,
    out_weight_ref,
    query_ref,
    key_ref,
    value_ref,
    gated_ref,
    sig_ref,
    grad_ref,
    score_ref,
    prob_ref,
    hidden_t_ref,
    cot_t_ref,
    hidden_ref,
    *,
    head_size,
):
    copies, length, _ = tokens_ref.shape
    inner = query_ref.shape[1]
    inverse_square_root = 1.0 / math.sqrt(head_size)
    for t in range(copies):
        part = slice(t * length, (t + 1) * length)
        scaled = scale_ref[t] * tokens_ref[t].astype(jnp.float32)
        hidden = normalize(scaled) * gain_ref[...]
        hidden_ref[part] = hidden.astype(jnp.bfloat16)
        hidden_t_ref[:, part] = hidden.T.astype(jnp.bfloat16)
        cot_t_ref[:, part] = cot_ref[t].astype(jnp.float32).T.astype(jnp.bfloat16)
    hidden = hidden_ref[...]
    query_ref[...] = dot_nt(hidden, weight_ref[0]).astype(jnp.bfloat16)
    key_ref[...] = dot_nt(hidden, weight_ref[1]).astype(jnp.bfloat16)
    value_ref[...] = dot_nt(hidden, weight_ref[2]).astype(jnp.bfloat16)
    sig = jax.nn.sigmoid(dot_nt(hidden, weight_ref[3]))
    sig_ref[...] = sig
    grad = dot_nt(cot_ref[...].reshape(copies * length, -1), out_weight_ref[...])
    grad_ref[...] = grad
    gated_ref[...] = (grad * sig).astype(jnp.bfloat16)
    head_of = lax.broadcasted_iota(jnp.int32, (length, inner), 1) // head_size
    for t in range(copies):
        part = slice(t * length, (t + 1) * length)
        query, key_rows, value, gated = (
            r[part] for r in (query_ref, key_ref, value_ref, gated_ref)
        )
        for h in range(score_ref.shape[1]):
            mine = head_of == h
            query_h = jnp.where(mine, query, jnp.zeros_like(query))
            gated_h = jnp.where(mine, gated, jnp.zeros_like(gated))
            score_ref[t, h] = dot_nt(query_h, key_rows) * inverse_square_root
            prob_ref[t, h] = dot_nt(gated_h, value)


def attention_kernel(
    here_ref,
    bias_ref,
    query_ref,
    key_ref,
    value_ref,
    gated_ref,
    sig_ref,
    grad_ref,
    score_ref,
    prob_ref,
    weight_ref,
    pair_ref,
    outs_ref,
    grads_ref,
    *refs,
    width,
    head_size,
):
    part_refs, (sums_ref, parts_ref) = refs[:-2], refs[-2:]
    stripes, cols, rows, _ = bias_ref.shape
    copies, heads, length, _ = score_ref.shape
    inner, hidden_width = weight_ref.shape[1:]
    share = length // cols
    lanes = lane_groups(length, width)
    head_of = lax.broadcasted_iota(jnp.int32, (length, inner), 1) // head_size
    inverse_square_root = 1.0 / math.sqrt(head_size)
    tiles = [
        bias_ref[:, col].astype(jnp.float32).reshape(length, LANES) for col in range(cols)
    ]
    bias = [
        merge([turn(tiles[col], col - h, width) for col in range(cols)], lanes)
        for h in range(heads)
    ]
    for t in range(copies):
        part = slice(t * length, (t + 1) * length)
        query, key_rows, value, gated = (
            r[part] for r in (query_ref, key_ref, value_ref, gated_ref)
        )
        attended = jnp.zeros((length, inner), jnp.float32)
        grad_query, grad_key, grad_value = attended, attended, attended
        for h in range(heads):
            mine = head_of == h
            query_h, key_h, value_h, gated_h = (
                jnp.where(mine, r, jnp.zeros_like(r)) for r in (query, key_rows, value, gated)
            )
            exponent = jnp.exp(score_ref[t, h] + bias[h])
            attention = exponent / jnp.sum(exponent, -1, keepdims=True)
            attention_b = attention.astype(jnp.bfloat16)
            grad_prob = prob_ref[t, h]
            grad_score = attention * (
                grad_prob - jnp.sum(attention * grad_prob, -1, keepdims=True)
            )
            sums_ref[h] = grad_score if t == 0 else sums_ref[h] + grad_score
            score_b = grad_score.astype(jnp.bfloat16)
            attended += dot_nn(attention_b, value_h)
            grad_query += dot_nn(score_b, key_h)
            grad_key += dot_tn(score_b, query_h)
            grad_value += dot_tn(attention_b, gated_h)
        sig = sig_ref[part]
        gated_out = (sig * attended).astype(jnp.bfloat16)
        grads = [
            (grad_query * inverse_square_root).astype(jnp.bfloat16),
            (grad_key * inverse_square_root).astype(jnp.bfloat16),
            grad_value.astype(jnp.bfloat16),
            (grad_ref[part] * attended * sig * (1.0 - sig)).astype(jnp.bfloat16),
        ]
        outs_ref[part] = gated_out
        for g in range(4):
            grads_ref[g, part] = grads[g]
        in_part = dot_nn(grads[0], weight_ref[0])
        for g in range(1, 4):
            in_part += dot_nn(grads[g], weight_ref[g])
        tail = jnp.concatenate(
            [gated_out[:, LANES:], jnp.zeros((length, 2 * LANES - inner), jnp.bfloat16)], axis=1
        )
        for first, values in (
            (0, in_part.astype(jnp.bfloat16)),
            (hidden_width, gated_out[:, :LANES]),
            (hidden_width + LANES, tail),
        ):
            size = values.shape[1]
            parts_ref[:, t, :, first : first + size] = values.reshape(cols, share, size)
    for k in range(cols):
        part_refs[k][...] = parts_ref[(here_ref[1] + k) % cols]
    for col in range(cols):
        pair_ref[:, col] = (
            merge([turn(sums_ref[h], h - col, width) for h in range(heads)], lanes)
            .astype(jnp.bfloat16)
            .reshape(stripes, rows, LANES)
        )


def weight_in_kernel(
    here_ref, hidden_t_ref, cot_t_ref, grads_ref, outs_ref, keep_ref, send_ref, wire_ref
):
    hidden_t = hidden_t_ref[...]
    chips, _, block, _ = wire_ref.shape

    def put(values, first, last):
        wire_ref[:, :, :, first * LANES : last * LANES] = values.astype(jnp.bfloat16).reshape(
            chips, 2, block, -1
        )

    weights = [dot_nn(hidden_t, grads_ref[g]) for g in range(4)]
    weights.append(dot_nn(cot_t_ref[...], outs_ref[...]))
    for g in range(5):
        put(weights[g][:, :LANES], g, g + 1)
    tails = [w[:, LANES:] for w in weights]
    tails.append(jnp.zeros_like(tails[0]))
    for g in range(3):
        put(jnp.concatenate(tails[2 * g : 2 * g + 2], axis=1), 5 + g, 6 + g)
    core = here_ref[0] % 2
    keep_ref[...] = wire_ref[:, core]
    send_ref[...] = wire_ref[:, 1 - core]


def weight_add_kernel(here_ref, keep_ref, got_ref, *refs):
    out_refs, sum_ref = refs[:-1], refs[-1]
    sum_ref[...] = (
        keep_ref[...].astype(jnp.float32) + got_ref[...].astype(jnp.float32)
    ).astype(jnp.bfloat16)
    chip = here_ref[0] // 2
    for k in range(len(out_refs)):
        out_refs[k][...] = sum_ref[chip ^ k]


def pair_back_kernel(
    in_ref, updated_ref, gain_ref, bias_weight_ref, grad_ref, weight_ref, *, width
):
    _, cols, rows, _ = in_ref.shape
    heads = bias_weight_ref.shape[0]
    groups = LANES // width
    total = jnp.sum(in_ref[...].astype(jnp.float32), 0).reshape(cols * rows, LANES)
    spread = dot_tn(
        head_gather(rows, cols, heads).astype(jnp.bfloat16), total.astype(jnp.bfloat16)
    )
    lanes = lane_groups(heads, width)
    head_group = lax.broadcasted_iota(jnp.int32, (heads, LANES), 0) % groups
    blocks = []
    for q in range(rows // groups):
        tiles = []
        for s in range(groups):
            i = q * groups + s
            tile = spread[i * heads : (i + 1) * heads]
            turned = tile
            for g in range(groups):
                turned = jnp.where(head_group == g, turn(tile, s - g, width), turned)
            tiles.append(turned)
        blocks.append(merge(tiles, lanes))
    grad_t = jnp.concatenate(blocks, axis=1).astype(jnp.bfloat16)
    updated = updated_ref[...]
    gain = gain_ref[...]
    grad_in = dot_tn(grad_t, bias_weight_ref[...])
    grad_ref[...] = norm_back(grad_in, updated, gain)
    bias_in = (normalize(updated) * gain).astype(jnp.bfloat16)
    weight = dot_nn(grad_t, bias_in).astype(jnp.bfloat16)
    for device in range(weight_ref.shape[0]):
        weight_ref[device] = weight


def token_out_kernel(here_ref, scale_ref, tokens_ref, cot_ref, gain_ref, weight_ref, *refs):
    out_ref, grad_ref, halves_ref, sums_ref = refs[-4:]
    copies, share, hidden_width = out_ref.shape
    inner = weight_ref.shape[0]
    others = halves_ref.shape[0]
    part_refs, mine_refs, other_refs = (
        refs[: others + 1],
        refs[others + 1 : 2 * others + 1],
        refs[2 * others + 1 : 3 * others + 1],
    )
    core = here_ref[0] % 2
    for k in range(others):
        halves_ref[k, core] = mine_refs[k][...]
        halves_ref[k, 1 - core] = other_refs[k][...]
    for k in range(others + 1):
        gated = part_refs[k][:, :, hidden_width : hidden_width + inner]
        weight = weight_ref[...] if k == 0 else halves_ref[k - 1].reshape(inner, hidden_width)
        product = dot_nn(gated.reshape(copies * share, inner), weight)
        sums_ref[...] = product if k == 0 else sums_ref[...] + product
    for t in range(copies):
        grad_hidden = part_refs[0][t, :, :hidden_width].astype(jnp.float32)
        for r in part_refs[1 : others + 1]:
            grad_hidden = grad_hidden + r[t, :, :hidden_width].astype(jnp.float32)
        scale = scale_ref[t]
        scaled = scale * tokens_ref[t].astype(jnp.float32)
        out_ref[t] = (scaled + sums_ref[t * share : (t + 1) * share]).astype(jnp.bfloat16)
        grad = cot_ref[t].astype(jnp.float32) + norm_back(grad_hidden, scaled, gain_ref[...])
        grad_ref[t] = (scale * grad).astype(jnp.bfloat16)


def weight_out_kernel(*refs):
    in_refs, (grad_ref, out_ref) = refs[:-2], refs[-2:]
    total = in_refs[0][...].astype(jnp.float32)
    for r in in_refs[1:]:
        total = total + r[...].astype(jnp.float32)
    half = LANES // 2
    for g in range(4):
        grad_ref[g, :, :LANES] = total[:, g * LANES : (g + 1) * LANES]
        first = (5 + g // 2) * LANES + (g % 2) * half
        grad_ref[g, :, LANES:] = total[:, first : first + half]
    rows = jnp.concatenate(
        [total[:, 4 * LANES : 5 * LANES], total[:, 7 * LANES : 8 * LANES]], axis=1
    )
    out_ref[...] = rows.T[: out_ref.shape[0]]


def fits(pair_repr, token_count, heads_all, inner, hidden_width, stripes, cols):
    rows, width, channels = pair_repr.shape
    groups = LANES // width if LANES % width == 0 else 0
    return (
        groups > 0
        and token_count == LANES
        and channels == LANES
        and channels == stripes * cols * groups
        and cols == groups
        and heads_all == cols * groups
        and rows % 16 == 0
        and stripes * rows == token_count
        and stripes % 2 == 0
        and stripes & (stripes - 1) == 0
        and inner == LANES + LANES // 2
        and hidden_width % (16 * stripes) == 0
    )


def shards(
    pair_repr,
    pair_mask,
    chain_id,
    tri_in_gain,
    tri_proj,
    tri_gate,
    tri_out_gain,
    tri_out,
    bias_gain,
    bias_weight,
    chain_bias,
    tokens,
    noise_level,
    attn_gain,
    attn_weight,
    out_weight,
    cotangent,
):
    stripe_axes = ("group", "row")
    all_axes = ("group", "row", "col")
    stripes = lax.axis_size(stripe_axes)
    cols = lax.axis_size("col")
    rows, width, channels = pair_repr.shape
    heads_all = bias_weight.shape[1]
    copies, length, hidden_width = tokens.shape
    inner = attn_weight.shape[2]
    if not fits(pair_repr, length, heads_all, inner, hidden_width, stripes, cols):
        return general_shards(
            pair_repr,
            pair_mask,
            chain_id,
            tri_in_gain,
            tri_proj,
            tri_gate,
            tri_out_gain,
            tri_out,
            bias_gain,
            bias_weight,
            chain_bias,
            tokens,
            noise_level,
            attn_gain,
            attn_weight,
            out_weight,
            cotangent,
        )
    head_size = hidden_width // heads_all
    devices = stripes * cols
    pairs = rows * width
    bf16, f32 = jnp.bfloat16, jnp.float32
    vmem = pl.BlockSpec(memory_space=pltpu.VMEM)
    smem = pl.BlockSpec(memory_space=pltpu.SMEM)
    row_index = lax.axis_index(stripe_axes)
    col_index = lax.axis_index("col")
    here = jnp.stack([row_index, col_index]).astype(jnp.int32)
    pair_flat = pair_repr.reshape(pairs, channels)
    scales = noise_scale(noise_level)
    weight_t = jnp.swapaxes(attn_weight, 1, 2)
    bias_weight_t = bias_weight.T

    def call(kernel, mib, out_shape, n_smem, n_vmem, scratch=(), **options):
        many = isinstance(out_shape, tuple)
        return pl.pallas_call(
            functools.partial(kernel, **options),
            out_shape=out_shape,
            in_specs=[smem] * n_smem + [vmem] * n_vmem,
            out_specs=(vmem,) * len(out_shape) if many else vmem,
            scratch_shapes=list(scratch),
            compiler_params=pltpu.CompilerParams(vmem_limit_bytes=mib << 20),
        )

    def exchange(values, axes):
        return lax.all_to_all(values, axes, 0, 0, tiled=True)

    def shift(values, k):
        return lax.ppermute(values, "col", [(i, (i + k) % cols) for i in range(cols)])

    projected = call(
        pair_in_kernel,
        8,
        whole((devices, 2, rows, LANES), bf16),
        0,
        4,
        [pltpu.VMEM((devices * rows, LANES), f32)],
    )(far(pair_flat), far(pair_mask), far(tri_in_gain[None]), far(tri_proj))
    sides = exchange(projected.reshape(devices, 2 * rows, LANES), all_axes)
    half = lax.dynamic_slice_in_dim(out_weight, row_index % 2 * (inner // 2), inner // 2, 0)
    halves = [shift(half, k) for k in range(1, cols)]
    tall = copies * length
    local = heads_all // cols
    query, key_rows, value, gated, gate_sig, grad_gated, scores, probs, hidden_t, cot_t = call(
        token_in_kernel,
        16,
        (
            *[pltpu.VMEM((tall, inner), bf16)] * 4,
            *[pltpu.VMEM((tall, inner), f32)] * 2,
            *[pltpu.VMEM((copies, local, length, length), f32)] * 2,
            *[pltpu.HBM((hidden_width, tall), bf16)] * 2,
        ),
        1,
        5,
        [pltpu.VMEM((tall, hidden_width), bf16)],
        head_size=head_size,
    )(
        scales, *map(far, (tokens, cotangent, attn_gain[None], weight_t, out_weight))
    )
    triangle = call(
        triangle_kernel, 8, whole((stripes, cols, rows, LANES), bf16), 0, 1, width=width
    )(sides.reshape(stripes, cols, 2, rows, LANES))
    triangle = exchange(triangle.reshape(devices, rows, LANES), all_axes)
    pair_next, updated, bias_tile = call(
        pair_out_kernel,
        8,
        (
            pltpu.HBM((pairs, channels), bf16),
            pltpu.HBM((pairs, channels), f32),
            whole((stripes, cols, rows, LANES), bf16),
        ),
        2,
        10,
        [pltpu.VMEM((devices * rows, LANES), f32)],
        width=width,
    )(
        here,
        chain_id,
        triangle,
        *map(
            far,
            (
                pair_flat,
                chain_id[None],
                tri_in_gain[None],
                tri_gate,
                tri_out_gain[None],
                tri_out,
                bias_gain[None],
                bias_weight_t,
                chain_bias[None],
            ),
        ),
    )
    head_bias = exchange(bias_tile.reshape(devices, rows, LANES), all_axes)
    share = length // cols
    part = pltpu.HBM((copies, share, hidden_width + 2 * LANES), bf16)
    bias_sums, outs, grads, *parts = call(
        attention_kernel,
        20,
        (
            pltpu.HBM((stripes, cols, rows, LANES), bf16),
            pltpu.HBM((tall, inner), bf16),
            pltpu.HBM((4, tall, inner), bf16),
            *[part] * cols,
        ),
        1,
        10,
        [
            pltpu.VMEM((local, length, length), f32),
            pltpu.VMEM((cols, copies, share, hidden_width + 2 * LANES), bf16),
        ],
        width=width,
        head_size=head_size,
    )(
        here,
        head_bias.reshape(stripes, cols, rows, LANES),
        *map(
            near,
            (query, key_rows, value, gated, gate_sig, grad_gated, scores, probs),
        ),
        far(weight_t),
    )
    bias_back = exchange(bias_sums.reshape(devices, rows, LANES), all_axes)
    received = [parts[0]] + [shift(parts[k], k) for k in range(1, cols)]
    others = []
    for k in range(1, cols):
        others.append(
            lax.ppermute(halves[k - 1], stripe_axes, [(i, i ^ 1) for i in range(stripes)])
        )
    chips = stripes // 2
    block = hidden_width // stripes
    keep, give = call(
        weight_in_kernel,
        16,
        (pltpu.VMEM((chips, block, 8 * LANES), bf16),) * 2,
        1,
        4,
        [pltpu.VMEM((chips, 2, block, 8 * LANES), bf16)],
    )(here, *map(far, (hidden_t, cot_t, grads, outs)))
    got = lax.ppermute(give, stripe_axes, [(i, i ^ 1) for i in range(stripes)])
    mine, *give = call(
        weight_add_kernel,
        12,
        (
            pltpu.HBM((block, 8 * LANES), bf16),
            *[pltpu.VMEM((block, 8 * LANES), bf16)] * (chips - 1),
        ),
        1,
        2,
        [pltpu.VMEM((chips, block, 8 * LANES), bf16)],
    )(here, near(keep), near(got))
    wires = [mine]
    for k in range(1, chips):
        wires.append(
            lax.ppermute(
                give[k - 1], stripe_axes, [(i, i ^ (2 * k)) for i in range(stripes)]
            )
        )
    pair_grad, weight_part = call(
        pair_back_kernel,
        8,
        (whole((pairs, channels), f32), whole((devices, heads_all, channels), bf16)),
        0,
        4,
        width=width,
    )(
        bias_back.reshape(stripes, cols, rows, LANES),
        *map(far, (updated, bias_gain[None], bias_weight_t)),
    )
    weight_part = exchange(weight_part, all_axes)
    bias_weight_grad = jnp.sum(weight_part.astype(f32), 0).T
    weight_grad, out_grad = call(
        weight_out_kernel,
        16,
        (
            whole((4, hidden_width // stripes, inner), f32),
            whole((inner, hidden_width // stripes), f32),
        ),
        0,
        chips,
    )(far(wires[0]), *map(near, wires[1:]))
    mine = pl.BlockSpec((copies, share, hidden_width), lambda i, here: (0, here[1], 0))
    fixed = lambda shape: pl.BlockSpec(shape, lambda i, here: (0,) * len(shape))
    denoised, token_grad = pl.pallas_call(
        token_out_kernel,
        grid_spec=pltpu.PrefetchScalarGridSpec(
            num_scalar_prefetch=1,
            grid=(1,),
            in_specs=[smem, mine, mine, fixed((1, hidden_width)), fixed((inner, hidden_width))]
            + [fixed((copies, share, hidden_width + 2 * LANES))] * cols
            + [fixed((inner // 2, hidden_width))] * (2 * cols - 2),
            out_specs=[fixed((copies, share, hidden_width))] * 2,
            scratch_shapes=[
                pltpu.VMEM((cols - 1, 2, inner // 2, hidden_width), bf16),
                pltpu.VMEM((copies * share, hidden_width), f32),
            ],
        ),
        out_shape=(whole((copies, share, hidden_width), bf16),) * 2,
        compiler_params=pltpu.CompilerParams(vmem_limit_bytes=16 << 20),
        name="token_out",
    )(
        here,
        scales,
        tokens,
        cotangent,
        attn_gain[None],
        out_weight,
        *received,
        *halves,
        *others,
    )
    return (
        pair_next.reshape(rows, width, channels),
        pair_grad.reshape(rows, width, channels),
        bias_weight_grad,
        denoised,
        token_grad,
        weight_grad,
        out_grad,
    )


def solution(mesh):
    return jax.shard_map(
        shards,
        mesh=mesh,
        in_specs=(
            P(("group", "row"), "col", None),
            P(("group", "row"), "col"),
            P(),
            P(),
            P(),
            P(),
            P(),
            P(),
            P(),
            P(),
            P(),
            P(("group", "row"), None, None),
            P(("group", "row")),
            P(),
            P(None, None, "col"),
            P("col", None),
            P(("group", "row"), None, None),
        ),
        out_specs=(
            P(("group", "row"), "col", None),
            P(("group", "row"), "col", None),
            P(),
            P(("group", "row"), "col", None),
            P(("group", "row"), "col", None),
            P(None, ("group", "row"), "col"),
            P("col", ("group", "row")),
        ),
        check_vma=False,
    )
```

```python
import functools
import math

import jax
import jax.numpy as jnp
from jax import lax
from jax.experimental import pallas as pl
from jax.experimental.pallas import tpu as pltpu
from jax.sharding import PartitionSpec as P


LEVELS = 200


EPSILON = 1e-05
SIGMA_LOW = 0.1
SIGMA_SPAN = 100.0


def normalize(values):
    average = jnp.mean(values, -1, keepdims=True)
    centred = values - average
    return centred * lax.rsqrt(jnp.mean(centred * centred, -1, keepdims=True) + EPSILON)


def norm_back(gradient, values, norm_gain):
    average = jnp.mean(values, -1, keepdims=True)
    centred = values - average
    inverse = lax.rsqrt(jnp.mean(centred * centred, -1, keepdims=True) + EPSILON)
    normed = centred * inverse
    weighted = gradient * norm_gain
    return inverse * (
        weighted
        - jnp.mean(weighted, -1, keepdims=True)
        - normed * jnp.mean(weighted * normed, -1, keepdims=True)
    )


def noise_scale(levels):
    sigma_vals = SIGMA_LOW * SIGMA_SPAN ** (levels.astype(jnp.float32) / (LEVELS - 1))
    return lax.rsqrt(1.0 + sigma_vals * sigma_vals)


def general_shards(
    pair_repr,
    pair_mask,
    chain_id,
    tri_in_gain,
    tri_proj,
    tri_gate,
    tri_out_gain,
    tri_out,
    bias_gain,
    bias_weight,
    chain_bias,
    tokens,
    noise_level,
    attn_gain,
    attn_weight,
    out_weight,
    cotangent,
):
    rows_here = pair_repr.shape[0]
    cols_here = pair_repr.shape[1]
    channels = pair_repr.shape[2]
    token_count = chain_id.shape[0]
    heads_all = bias_weight.shape[1]
    hidden_width = attn_gain.shape[0]
    head_size = hidden_width // heads_all
    inverse_square_root = 1.0 / math.sqrt(head_size)
    row_index = lax.axis_index(("group", "row"))
    col_index = lax.axis_index("col")
    pair_tile = pair_repr.astype(jnp.float32)
    pair_in = (normalize(pair_tile) * tri_in_gain).astype(jnp.bfloat16)
    flat_in = pair_in.reshape(-1, channels)
    projected = jnp.dot(flat_in, tri_proj, preferred_element_type=jnp.float32).reshape(
        rows_here, cols_here, 4, channels
    )
    mask_tile = pair_mask.astype(jnp.float32)[:, :, None]
    left_proj = (jax.nn.sigmoid(projected[:, :, 0]) * projected[:, :, 1] * mask_tile).astype(
        jnp.bfloat16
    )
    right_proj = (jax.nn.sigmoid(projected[:, :, 2]) * projected[:, :, 3] * mask_tile).astype(
        jnp.bfloat16
    )
    gate_act = jax.nn.sigmoid(
        jnp.dot(flat_in, tri_gate, preferred_element_type=jnp.float32)
    ).reshape(rows_here, cols_here, channels)
    left_major = jnp.transpose(left_proj, (2, 0, 1))
    right_major = jnp.transpose(right_proj, (2, 0, 1))
    partial_rows = jnp.einsum(
        "cjk,cik->cji",
        lax.all_gather(right_major, ("group", "row"), axis=1, tiled=True),
        left_major,
        preferred_element_type=jnp.float32,
    )
    summed = lax.psum_scatter(partial_rows, "col", scatter_dimension=1, tiled=True)
    triangle = jnp.transpose(summed, (2, 1, 0))
    tri_normed = (normalize(triangle) * tri_out_gain).astype(jnp.bfloat16)
    update = jnp.dot(
        tri_normed.reshape(-1, channels), tri_out, preferred_element_type=jnp.float32
    ).reshape(rows_here, cols_here, channels)
    updated = pair_tile + gate_act * update
    bias_in = (normalize(updated) * bias_gain).astype(jnp.bfloat16)
    flat_bias = bias_in.reshape(-1, channels)
    bias_tile = jnp.dot(flat_bias, bias_weight, preferred_element_type=jnp.float32).reshape(
        rows_here, cols_here, heads_all
    )
    row_chain = lax.dynamic_slice_in_dim(chain_id, row_index * rows_here, rows_here)
    col_chain = lax.dynamic_slice_in_dim(chain_id, col_index * cols_here, cols_here)
    same_chain = (row_chain[:, None] == col_chain[None, :]).astype(jnp.float32)
    bias_tile = bias_tile + same_chain[:, :, None] * chain_bias
    bias_major = jnp.transpose(bias_tile.astype(jnp.bfloat16), (2, 0, 1))
    head_rows = lax.all_to_all(bias_major, "col", split_axis=0, concat_axis=2, tiled=True)
    per_head_bias = lax.all_gather(head_rows, ("group", "row"), axis=1, tiled=True).astype(
        jnp.float32
    )
    local_heads = per_head_bias.shape[0]
    scales = noise_scale(noise_level)

    def one_copy(carried, inputs):
        bias_sums, weight_sums, output_sums = carried
        token_rows, cot_rows, scaling = inputs
        sequence_length = token_rows.shape[0]
        scaled = scaling * token_rows.astype(jnp.float32)
        hidden = (normalize(scaled) * attn_gain).astype(jnp.bfloat16)
        projections = jnp.einsum(
            "nd,gde->gne", hidden, attn_weight, preferred_element_type=jnp.float32
        )
        query_rows = (
            projections[0].astype(jnp.bfloat16).reshape(sequence_length, local_heads, head_size)
        )
        key_matrix = (
            projections[1].astype(jnp.bfloat16).reshape(sequence_length, local_heads, head_size)
        )
        value_rows = (
            projections[2].astype(jnp.bfloat16).reshape(sequence_length, local_heads, head_size)
        )
        gate_sig = jax.nn.sigmoid(projections[3])
        logit_scores = (
            jnp.einsum("fuc,suc->ufs", query_rows, key_matrix, preferred_element_type=jnp.float32)
            * inverse_square_root
            + per_head_bias
        )
        exponent = jnp.exp(logit_scores)
        attention = exponent / jnp.sum(exponent, -1, keepdims=True)
        attention_probs = attention.astype(jnp.bfloat16)
        attended_rows = jnp.einsum(
            "vkq,qvy->kvy", attention_probs, value_rows, preferred_element_type=jnp.float32
        ).reshape(sequence_length, -1)
        gated_out = (gate_sig * attended_rows).astype(jnp.bfloat16)
        grad_gated = jnp.dot(cot_rows, out_weight.T, preferred_element_type=jnp.float32)
        grad_gate = grad_gated * attended_rows * gate_sig * (1.0 - gate_sig)
        attended_gradient = (
            (grad_gated * gate_sig)
            .astype(jnp.bfloat16)
            .reshape(sequence_length, local_heads, head_size)
        )
        probability_gradient = jnp.einsum(
            "fuc,suc->ufs", attended_gradient, value_rows, preferred_element_type=jnp.float32
        )
        value_gradient = jnp.einsum(
            "avj,vat->jat", attention_probs, attended_gradient, preferred_element_type=jnp.float32
        )
        grad_score = attention * (
            probability_gradient - jnp.sum(attention * probability_gradient, -1, keepdims=True)
        )
        score_gradient = grad_score.astype(jnp.bfloat16)
        query_gradient = (
            jnp.einsum(
                "vkq,qvy->kvy", score_gradient, key_matrix, preferred_element_type=jnp.float32
            )
            * inverse_square_root
        )
        key_gradient = (
            jnp.einsum(
                "avj,vat->jat", score_gradient, query_rows, preferred_element_type=jnp.float32
            )
            * inverse_square_root
        )
        grads = jnp.stack(
            [
                query_gradient.reshape(sequence_length, -1),
                key_gradient.reshape(sequence_length, -1),
                value_gradient.reshape(sequence_length, -1),
                grad_gate,
            ]
        ).astype(jnp.bfloat16)
        weight_sums = weight_sums + jnp.einsum(
            "nd,gne->gde", hidden, grads, preferred_element_type=jnp.float32
        )
        output_sums = output_sums + jnp.dot(
            gated_out.T, cot_rows, preferred_element_type=jnp.float32
        )
        return ((bias_sums + grad_score, weight_sums, output_sums), (gated_out, grads))

    start_sums = (
        jnp.zeros((local_heads, token_count, token_count), jnp.float32),
        jnp.zeros(attn_weight.shape, jnp.float32),
        jnp.zeros(out_weight.shape, jnp.float32),
    )
    final_sums, stacked = lax.scan(one_copy, start_sums, (tokens, cotangent, scales))
    bias_sums, weight_sums, output_sums = final_sums
    gated_all, grads_all = stacked
    token_share = token_count // lax.axis_size("col")
    attn_parts = jnp.einsum(
        "tnd,de->tne", gated_all, out_weight, preferred_element_type=jnp.float32
    )
    hidden_parts = jnp.einsum(
        "tgne,gde->tnd", grads_all, attn_weight, preferred_element_type=jnp.float32
    )
    attn_out, grad_hidden = (
        lax.psum_scatter(attn_parts, "col", scatter_dimension=1, tiled=True),
        lax.psum_scatter(hidden_parts, "col", scatter_dimension=1, tiled=True),
    )
    first_token = col_index * token_share
    token_mine = lax.dynamic_slice_in_dim(tokens, first_token, token_share, 1)
    cot_mine = lax.dynamic_slice_in_dim(cotangent, first_token, token_share, 1)
    scaled_mine = scales[:, None, None] * token_mine.astype(jnp.float32)
    denoised = (scaled_mine + attn_out).astype(jnp.bfloat16)
    grad_scaled = cot_mine.astype(jnp.float32) + norm_back(grad_hidden, scaled_mine, attn_gain)
    token_grad = (scales[:, None, None] * grad_scaled).astype(jnp.bfloat16)
    bias_rows_sum, out_grad, weight_grad = (
        lax.psum_scatter(bias_sums, ("group", "row"), scatter_dimension=1, tiled=True),
        lax.psum_scatter(output_sums, ("group", "row"), scatter_dimension=1, tiled=True),
        lax.psum_scatter(weight_sums, ("group", "row"), scatter_dimension=1, tiled=True),
    )
    bias_back = lax.all_to_all(bias_rows_sum, "col", split_axis=2, concat_axis=0, tiled=True)
    grad_bias = jnp.transpose(bias_back, (1, 2, 0)).reshape(-1, heads_all)
    grad_in = jnp.dot(
        grad_bias, bias_weight.astype(jnp.float32).T, precision=lax.Precision.HIGHEST
    ).reshape(rows_here, cols_here, channels)
    pair_grad = norm_back(grad_in, updated, bias_gain)
    weight_part = jnp.dot(
        flat_bias.astype(jnp.float32).T, grad_bias, precision=lax.Precision.HIGHEST
    )
    bias_weight_grad = lax.psum(weight_part, ("group", "row", "col"))
    return (
        updated.astype(jnp.bfloat16),
        pair_grad,
        bias_weight_grad,
        denoised,
        token_grad,
        weight_grad,
        out_grad,
    )


LANES = 128


def dot_nn(a, b, **kw):
    return lax.dot_general(a, b, (((1,), (0,)), ((), ())), preferred_element_type=jnp.float32, **kw)


def dot_nt(a, b, **kw):
    return lax.dot_general(a, b, (((1,), (1,)), ((), ())), preferred_element_type=jnp.float32, **kw)


def dot_tn(a, b, **kw):
    return lax.dot_general(a, b, (((0,), (0,)), ((), ())), preferred_element_type=jnp.float32, **kw)


def turn(values, groups, width):
    shift = (groups * width) % LANES
    return values if shift == 0 else pltpu.roll(values, shift, 1)


def merge(pieces, lane_group):
    merged = pieces[0]
    for g in range(1, len(pieces)):
        merged = jnp.where(lane_group == g, pieces[g], merged)
    return merged


def lane_groups(rows, width):
    return lax.broadcasted_iota(jnp.int32, (rows, LANES), 1) // width


def channel_order(channels, devices):
    r = lax.broadcasted_iota(jnp.int32, (channels, channels), 0)
    c = lax.broadcasted_iota(jnp.int32, (channels, channels), 1)
    return (r % devices) * (channels // devices) + r // devices == c


def whole(shape, dtype):
    return jax.ShapeDtypeStruct(shape, dtype)


def far(values):
    return pltpu.with_memory_space_constraint(values, pltpu.HBM)


def near(values):
    return pltpu.with_memory_space_constraint(values, pltpu.VMEM)


def pair_in_kernel(pair_ref, mask_ref, gain_ref, proj_ref, out_ref, rows_ref):
    devices = out_ref.shape[0]
    rows, width = mask_ref.shape
    channels = pair_ref.shape[1]
    groups = LANES // width
    pair_in = (normalize(pair_ref[...].astype(jnp.float32)) * gain_ref[...]).astype(jnp.bfloat16)
    order = channel_order(channels, devices).astype(jnp.float32).astype(jnp.bfloat16)
    lanes = lane_groups(devices, width)
    mask = jnp.concatenate([mask_ref[...].astype(jnp.float32)] * groups, axis=1)
    for side in range(2):
        first = 2 * side * channels
        gate_t = dot_nt(order, proj_ref[:, first : first + channels]).astype(jnp.bfloat16)
        value_t = dot_nt(order, proj_ref[:, first + channels : first + 2 * channels]).astype(
            jnp.bfloat16
        )
        product = jax.nn.sigmoid(dot_nt(gate_t, pair_in)) * dot_nt(value_t, pair_in)
        for i in range(rows):
            q, s = divmod(i, groups)
            tile = merge(
                [
                    turn(
                        product[g * devices : (g + 1) * devices, q * LANES : (q + 1) * LANES],
                        g - s,
                        width,
                    )
                    for g in range(groups)
                ],
                lanes,
            )
            rows_ref[pl.ds(i, devices, stride=rows), :] = tile * mask[i : i + 1]
        out_ref[:, side] = rows_ref[...].astype(jnp.bfloat16).reshape(devices, rows, LANES)


def triangle_kernel(in_ref, out_ref, *, width):
    stripes, cols, _, rows, _ = in_ref.shape
    groups = LANES // width
    tokens = stripes * rows
    lanes = lane_groups(tokens, width)
    totals = [jnp.zeros((tokens, LANES), jnp.float32) for _ in range(groups)]
    for col in range(cols):
        left = in_ref[:, col, 0].reshape(tokens, LANES)
        right = in_ref[:, col, 1].reshape(tokens, LANES)
        for g in range(groups):
            totals[g] += dot_nt(jnp.where(lanes == g, left, jnp.zeros_like(left)), right)
    for col in range(cols):
        out_ref[:, col] = (
            merge([turn(totals[g], g - col, width) for g in range(groups)], lanes)
            .astype(jnp.bfloat16)
            .reshape(stripes, rows, LANES)
        )


def pair_gate_kernel(
    pair_ref, gain_ref, gate_ref, out_gain_ref, out_weight_ref, out_ref, *, devices
):
    pairs, channels = pair_ref.shape
    pair_in = (normalize(pair_ref[...].astype(jnp.float32)) * gain_ref[...]).astype(jnp.bfloat16)
    out_ref[:pairs] = jax.nn.sigmoid(dot_nn(pair_in, gate_ref[...]))
    order = channel_order(channels, devices)
    gain_t = jnp.sum(jnp.where(order, out_gain_ref[...], 0.0), axis=1, keepdims=True)
    order_b = order.astype(jnp.float32).astype(jnp.bfloat16)
    out_ref[pairs:] = dot_nn(order_b, out_weight_ref[...]) * gain_t


def pair_out_kernel(
    here_ref,
    chain_ref,
    in_ref,
    pair_ref,
    chain_row_ref,
    gate_ref,
    bias_gain_ref,
    bias_weight_ref,
    chain_bias_ref,
    next_ref,
    updated_ref,
    bias_ref,
    rows_ref,
    *,
    width,
):
    devices, rows, _ = in_ref.shape
    stripes, cols = bias_ref.shape[:2]
    channels = pair_ref.shape[1]
    heads = bias_weight_ref.shape[0]
    groups = LANES // width

    def all_lanes(sums):
        total = sums
        for g in range(1, groups):
            total = total + turn(sums, g, width)
        return total

    triangle = in_ref[...].astype(jnp.float32)
    average = all_lanes(jnp.sum(triangle, 0)) * (1.0 / channels)
    centred = triangle - average
    inverse = lax.rsqrt(all_lanes(jnp.sum(centred * centred, 0)) * (1.0 / channels) + EPSILON)
    rows_ref[...] = (centred * inverse).reshape(devices * rows, LANES)
    lanes = lane_groups(devices, width)
    blocks = []
    for q in range(rows // groups):
        tiles = [
            rows_ref[pl.ds(q * groups + s, devices, stride=rows), :] for s in range(groups)
        ]
        blocks.append(
            jnp.concatenate(
                [
                    merge([turn(tiles[s], s - g, width) for s in range(groups)], lanes)
                    for g in range(groups)
                ],
                axis=0,
            )
        )
    normed_t = jnp.concatenate(blocks, axis=1)
    pairs = pair_ref.shape[0]
    update = dot_tn(normed_t.astype(jnp.bfloat16), gate_ref[pairs:].astype(jnp.bfloat16))
    updated = pair_ref[...].astype(jnp.float32) + gate_ref[:pairs] * update
    updated_ref[...] = updated
    next_ref[...] = updated.astype(jnp.bfloat16)
    bias_in = (normalize(updated) * bias_gain_ref[...]).astype(jnp.bfloat16)
    unit = lax.broadcasted_iota(jnp.int32, (heads, heads), 0) == lax.broadcasted_iota(
        jnp.int32, (heads, heads), 1
    )
    chain_t = jnp.sum(jnp.where(unit, chain_bias_ref[...], 0.0), axis=1, keepdims=True)
    bias_t = dot_nt(bias_weight_ref[...], bias_in)
    lanes_h = lane_groups(heads, width)
    chain_row = jnp.broadcast_to(chain_row_ref[...], (heads, LANES))
    col_chain = merge(
        [
            pltpu.roll(chain_row, (g + cols - here_ref[1]) % cols * width, 1)
            for g in range(groups)
        ],
        lanes_h,
    )
    head_group = lax.broadcasted_iota(jnp.int32, (heads, LANES), 0) % groups
    spread = []
    for i in range(rows):
        q, s = divmod(i, groups)
        block = bias_t[:, q * LANES : (q + 1) * LANES]
        tile = jnp.zeros_like(block)
        for g in range(groups):
            tile = jnp.where(
                (lanes_h == g) & (head_group == g), turn(block, g - s, width), tile
            )
        row_chain = chain_ref[here_ref[0] * rows + i]
        extra = jnp.where((col_chain == row_chain) & (lanes_h == head_group), chain_t, 0.0)
        spread.append(tile + extra)
    spread = jnp.concatenate(spread, axis=0).astype(jnp.bfloat16)
    packed = dot_nn(head_gather(rows, cols, heads).astype(jnp.bfloat16), spread)
    packed = packed.astype(jnp.bfloat16).reshape(cols, rows, LANES)
    for stripe in range(stripes):
        bias_ref[stripe] = packed


def head_gather(rows, cols, heads):
    a = lax.broadcasted_iota(jnp.int32, (cols * rows, rows * heads), 0)
    b = lax.broadcasted_iota(jnp.int32, (cols * rows, rows * heads), 1)
    return ((a % rows == b // heads) & (a // rows == (b % heads) // (heads // cols))).astype(
        jnp.float32
    )


def token_in_kernel(
    scale_ref,
    tokens_ref,
    cot_ref,
    gain_ref,
    weight_ref,
    out_weight_ref,
    query_ref,
    key_ref,
    value_ref,
    gated_ref,
    sig_ref,
    grad_ref,
    score_ref,
    prob_ref,
    hidden_t_ref,
    cot_t_ref,
    hidden_ref,
    *,
    head_size,
):
    copies, length, _ = tokens_ref.shape
    inner = query_ref.shape[1]
    inverse_square_root = 1.0 / math.sqrt(head_size)
    for t in range(copies):
        part = slice(t * length, (t + 1) * length)
        scaled = scale_ref[t] * tokens_ref[t].astype(jnp.float32)
        hidden = normalize(scaled) * gain_ref[...]
        hidden_ref[part] = hidden.astype(jnp.bfloat16)
        hidden_t_ref[:, part] = hidden.T.astype(jnp.bfloat16)
        cot_t_ref[:, part] = cot_ref[t].astype(jnp.float32).T.astype(jnp.bfloat16)
    hidden = hidden_ref[...]
    query_ref[...] = dot_nt(hidden, weight_ref[0]).astype(jnp.bfloat16)
    key_ref[...] = dot_nt(hidden, weight_ref[1]).astype(jnp.bfloat16)
    value_ref[...] = dot_nt(hidden, weight_ref[2]).astype(jnp.bfloat16)
    sig = jax.nn.sigmoid(dot_nt(hidden, weight_ref[3]))
    sig_ref[...] = sig
    grad = dot_nt(cot_ref[...].reshape(copies * length, -1), out_weight_ref[...])
    grad_ref[...] = grad
    gated_ref[...] = (grad * sig).astype(jnp.bfloat16)
    head_of = lax.broadcasted_iota(jnp.int32, (length, inner), 1) // head_size
    for t in range(copies):
        part = slice(t * length, (t + 1) * length)
        query, key_rows, value, gated = (
            r[part] for r in (query_ref, key_ref, value_ref, gated_ref)
        )
        for h in range(score_ref.shape[1]):
            mine = head_of == h
            query_h = jnp.where(mine, query, jnp.zeros_like(query))
            gated_h = jnp.where(mine, gated, jnp.zeros_like(gated))
            score_ref[t, h] = dot_nt(query_h, key_rows) * inverse_square_root
            prob_ref[t, h] = dot_nt(gated_h, value)


def attention_kernel(
    here_ref,
    bias_ref,
    query_ref,
    key_ref,
    value_ref,
    gated_ref,
    sig_ref,
    grad_ref,
    score_ref,
    prob_ref,
    weight_ref,
    pair_ref,
    outs_ref,
    grads_ref,
    *refs,
    width,
    head_size,
):
    part_refs, (sums_ref, parts_ref) = refs[:-2], refs[-2:]
    stripes, cols, rows, _ = bias_ref.shape
    copies, heads, length, _ = score_ref.shape
    inner, hidden_width = weight_ref.shape[1:]
    share = length // cols
    lanes = lane_groups(length, width)
    head_of = lax.broadcasted_iota(jnp.int32, (length, inner), 1) // head_size
    inverse_square_root = 1.0 / math.sqrt(head_size)
    tiles = [
        bias_ref[:, col].astype(jnp.float32).reshape(length, LANES) for col in range(cols)
    ]
    bias = [
        merge([turn(tiles[col], col - h, width) for col in range(cols)], lanes)
        for h in range(heads)
    ]
    for t in range(copies):
        part = slice(t * length, (t + 1) * length)
        query, key_rows, value, gated = (
            r[part] for r in (query_ref, key_ref, value_ref, gated_ref)
        )
        attended = jnp.zeros((length, inner), jnp.float32)
        grad_query, grad_key, grad_value = attended, attended, attended
        for h in range(heads):
            mine = head_of == h
            query_h, key_h, value_h, gated_h = (
                jnp.where(mine, r, jnp.zeros_like(r)) for r in (query, key_rows, value, gated)
            )
            exponent = jnp.exp(score_ref[t, h] + bias[h])
            attention = exponent / jnp.sum(exponent, -1, keepdims=True)
            attention_b = attention.astype(jnp.bfloat16)
            grad_prob = prob_ref[t, h]
            grad_score = attention * (
                grad_prob - jnp.sum(attention * grad_prob, -1, keepdims=True)
            )
            sums_ref[h] = grad_score if t == 0 else sums_ref[h] + grad_score
            score_b = grad_score.astype(jnp.bfloat16)
            attended += dot_nn(attention_b, value_h)
            grad_query += dot_nn(score_b, key_h)
            grad_key += dot_tn(score_b, query_h)
            grad_value += dot_tn(attention_b, gated_h)
        sig = sig_ref[part]
        gated_out = (sig * attended).astype(jnp.bfloat16)
        grads = [
            (grad_query * inverse_square_root).astype(jnp.bfloat16),
            (grad_key * inverse_square_root).astype(jnp.bfloat16),
            grad_value.astype(jnp.bfloat16),
            (grad_ref[part] * attended * sig * (1.0 - sig)).astype(jnp.bfloat16),
        ]
        outs_ref[part] = gated_out
        for g in range(4):
            grads_ref[g, part] = grads[g]
        in_part = dot_nn(grads[0], weight_ref[0])
        for g in range(1, 4):
            in_part += dot_nn(grads[g], weight_ref[g])
        tail = jnp.concatenate(
            [gated_out[:, LANES:], jnp.zeros((length, 2 * LANES - inner), jnp.bfloat16)], axis=1
        )
        for first, values in (
            (0, in_part.astype(jnp.bfloat16)),
            (hidden_width, gated_out[:, :LANES]),
            (hidden_width + LANES, tail),
        ):
            size = values.shape[1]
            parts_ref[:, t, :, first : first + size] = values.reshape(cols, share, size)
    for k in range(cols):
        part_refs[k][...] = parts_ref[(here_ref[1] + k) % cols]
    for col in range(cols):
        pair_ref[:, col] = (
            merge([turn(sums_ref[h], h - col, width) for h in range(heads)], lanes)
            .astype(jnp.bfloat16)
            .reshape(stripes, rows, LANES)
        )


def weight_in_kernel(
    here_ref, hidden_t_ref, cot_t_ref, grads_ref, outs_ref, keep_ref, send_ref, wire_ref
):
    hidden_t = hidden_t_ref[...]
    chips, _, block, _ = wire_ref.shape

    def put(values, first, last):
        wire_ref[:, :, :, first * LANES : last * LANES] = values.astype(jnp.bfloat16).reshape(
            chips, 2, block, -1
        )

    weights = [dot_nn(hidden_t, grads_ref[g]) for g in range(4)]
    weights.append(dot_nn(cot_t_ref[...], outs_ref[...]))
    for g in range(5):
        put(weights[g][:, :LANES], g, g + 1)
    tails = [w[:, LANES:] for w in weights]
    tails.append(jnp.zeros_like(tails[0]))
    for g in range(3):
        put(jnp.concatenate(tails[2 * g : 2 * g + 2], axis=1), 5 + g, 6 + g)
    core = here_ref[0] % 2
    keep_ref[...] = wire_ref[:, core]
    send_ref[...] = wire_ref[:, 1 - core]


def weight_add_kernel(here_ref, keep_ref, got_ref, *refs):
    out_refs, sum_ref = refs[:-1], refs[-1]
    sum_ref[...] = (
        keep_ref[...].astype(jnp.float32) + got_ref[...].astype(jnp.float32)
    ).astype(jnp.bfloat16)
    chip = here_ref[0] // 2
    for k in range(len(out_refs)):
        out_refs[k][...] = sum_ref[chip ^ k]


def pair_back_kernel(
    in_ref, updated_ref, gain_ref, bias_weight_ref, grad_ref, weight_ref, *, width
):
    _, cols, rows, _ = in_ref.shape
    heads = bias_weight_ref.shape[0]
    groups = LANES // width
    total = jnp.sum(in_ref[...].astype(jnp.float32), 0).reshape(cols * rows, LANES)
    spread = dot_tn(
        head_gather(rows, cols, heads).astype(jnp.bfloat16), total.astype(jnp.bfloat16)
    )
    lanes = lane_groups(heads, width)
    head_group = lax.broadcasted_iota(jnp.int32, (heads, LANES), 0) % groups
    blocks = []
    for q in range(rows // groups):
        tiles = []
        for s in range(groups):
            i = q * groups + s
            tile = spread[i * heads : (i + 1) * heads]
            turned = tile
            for g in range(groups):
                turned = jnp.where(head_group == g, turn(tile, s - g, width), turned)
            tiles.append(turned)
        blocks.append(merge(tiles, lanes))
    grad_t = jnp.concatenate(blocks, axis=1).astype(jnp.bfloat16)
    updated = updated_ref[...]
    gain = gain_ref[...]
    grad_in = dot_tn(grad_t, bias_weight_ref[...])
    grad_ref[...] = norm_back(grad_in, updated, gain)
    bias_in = (normalize(updated) * gain).astype(jnp.bfloat16)
    weight = dot_nn(grad_t, bias_in).astype(jnp.bfloat16)
    for device in range(weight_ref.shape[0]):
        weight_ref[device] = weight


def token_out_kernel(here_ref, scale_ref, tokens_ref, cot_ref, gain_ref, weight_ref, *refs):
    out_ref, grad_ref, halves_ref, sums_ref = refs[-4:]
    copies, share, hidden_width = out_ref.shape
    inner = weight_ref.shape[0]
    others = halves_ref.shape[0]
    part_refs, mine_refs, other_refs = (
        refs[: others + 1],
        refs[others + 1 : 2 * others + 1],
        refs[2 * others + 1 : 3 * others + 1],
    )
    core = here_ref[0] % 2
    for k in range(others):
        halves_ref[k, core] = mine_refs[k][...]
        halves_ref[k, 1 - core] = other_refs[k][...]
    for k in range(others + 1):
        gated = part_refs[k][:, :, hidden_width : hidden_width + inner]
        weight = weight_ref[...] if k == 0 else halves_ref[k - 1].reshape(inner, hidden_width)
        product = dot_nn(gated.reshape(copies * share, inner), weight)
        sums_ref[...] = product if k == 0 else sums_ref[...] + product
    for t in range(copies):
        grad_hidden = part_refs[0][t, :, :hidden_width].astype(jnp.float32)
        for r in part_refs[1 : others + 1]:
            grad_hidden = grad_hidden + r[t, :, :hidden_width].astype(jnp.float32)
        scale = scale_ref[t]
        scaled = scale * tokens_ref[t].astype(jnp.float32)
        out_ref[t] = (scaled + sums_ref[t * share : (t + 1) * share]).astype(jnp.bfloat16)
        grad = cot_ref[t].astype(jnp.float32) + norm_back(grad_hidden, scaled, gain_ref[...])
        grad_ref[t] = (scale * grad).astype(jnp.bfloat16)


def weight_out_kernel(*refs):
    in_refs, (grad_ref, out_ref) = refs[:-2], refs[-2:]
    total = in_refs[0][...].astype(jnp.float32)
    for r in in_refs[1:]:
        total = total + r[...].astype(jnp.float32)
    half = LANES // 2
    for g in range(4):
        grad_ref[g, :, :LANES] = total[:, g * LANES : (g + 1) * LANES]
        first = (5 + g // 2) * LANES + (g % 2) * half
        grad_ref[g, :, LANES:] = total[:, first : first + half]
    rows = jnp.concatenate(
        [total[:, 4 * LANES : 5 * LANES], total[:, 7 * LANES : 8 * LANES]], axis=1
    )
    out_ref[...] = rows.T[: out_ref.shape[0]]


def fits(pair_repr, token_count, heads_all, inner, hidden_width, stripes, cols):
    rows, width, channels = pair_repr.shape
    groups = LANES // width if LANES % width == 0 else 0
    return (
        groups > 0
        and token_count == LANES
        and channels == LANES
        and channels == stripes * cols * groups
        and cols == groups
        and heads_all == cols * groups
        and rows % 16 == 0
        and stripes * rows == token_count
        and stripes % 2 == 0
        and stripes & (stripes - 1) == 0
        and inner == LANES + LANES // 2
        and hidden_width % (16 * stripes) == 0
    )


def shards(
    pair_repr,
    pair_mask,
    chain_id,
    tri_in_gain,
    tri_proj,
    tri_gate,
    tri_out_gain,
    tri_out,
    bias_gain,
    bias_weight,
    chain_bias,
    tokens,
    noise_level,
    attn_gain,
    attn_weight,
    out_weight,
    cotangent,
):
    stripe_axes = ("group", "row")
    all_axes = ("group", "row", "col")
    stripes = lax.axis_size(stripe_axes)
    cols = lax.axis_size("col")
    rows, width, channels = pair_repr.shape
    heads_all = bias_weight.shape[1]
    copies, length, hidden_width = tokens.shape
    inner = attn_weight.shape[2]
    if not fits(pair_repr, length, heads_all, inner, hidden_width, stripes, cols):
        return general_shards(
            pair_repr,
            pair_mask,
            chain_id,
            tri_in_gain,
            tri_proj,
            tri_gate,
            tri_out_gain,
            tri_out,
            bias_gain,
            bias_weight,
            chain_bias,
            tokens,
            noise_level,
            attn_gain,
            attn_weight,
            out_weight,
            cotangent,
        )
    head_size = hidden_width // heads_all
    devices = stripes * cols
    pairs = rows * width
    bf16, f32 = jnp.bfloat16, jnp.float32
    vmem = pl.BlockSpec(memory_space=pltpu.VMEM)
    smem = pl.BlockSpec(memory_space=pltpu.SMEM)
    row_index = lax.axis_index(stripe_axes)
    col_index = lax.axis_index("col")
    here = jnp.stack([row_index, col_index]).astype(jnp.int32)
    pair_flat = pair_repr.reshape(pairs, channels)
    scales = noise_scale(noise_level)
    weight_t = jnp.swapaxes(attn_weight, 1, 2)
    bias_weight_t = bias_weight.T

    def call(kernel, mib, out_shape, n_smem, n_vmem, scratch=(), **options):
        many = isinstance(out_shape, tuple)
        return pl.pallas_call(
            functools.partial(kernel, **options),
            out_shape=out_shape,
            in_specs=[smem] * n_smem + [vmem] * n_vmem,
            out_specs=(vmem,) * len(out_shape) if many else vmem,
            scratch_shapes=list(scratch),
            compiler_params=pltpu.CompilerParams(vmem_limit_bytes=mib << 20),
        )

    def exchange(values, axes):
        return lax.all_to_all(values, axes, 0, 0, tiled=True)

    def shift(values, k):
        return lax.ppermute(values, "col", [(i, (i + k) % cols) for i in range(cols)])

    projected = call(
        pair_in_kernel,
        8,
        whole((devices, 2, rows, LANES), bf16),
        0,
        4,
        [pltpu.VMEM((devices * rows, LANES), f32)],
    )(far(pair_flat), far(pair_mask), far(tri_in_gain[None]), far(tri_proj))
    sides = exchange(projected.reshape(devices, 2 * rows, LANES), all_axes)
    half = lax.dynamic_slice_in_dim(out_weight, row_index % 2 * (inner // 2), inner // 2, 0)
    halves = [shift(half, k) for k in range(1, cols)]
    tall = copies * length
    local = heads_all // cols
    query, key_rows, value, gated, gate_sig, grad_gated, scores, probs, hidden_t, cot_t = call(
        token_in_kernel,
        16,
        (
            *[pltpu.VMEM((tall, inner), bf16)] * 4,
            *[pltpu.VMEM((tall, inner), f32)] * 2,
            *[pltpu.VMEM((copies, local, length, length), f32)] * 2,
            *[pltpu.HBM((hidden_width, tall), bf16)] * 2,
        ),
        1,
        5,
        [pltpu.VMEM((tall, hidden_width), bf16)],
        head_size=head_size,
    )(
        scales, *map(far, (tokens, cotangent, attn_gain[None], weight_t, out_weight))
    )
    triangle = call(
        triangle_kernel, 8, whole((stripes, cols, rows, LANES), bf16), 0, 1, width=width
    )(sides.reshape(stripes, cols, 2, rows, LANES))
    triangle = exchange(triangle.reshape(devices, rows, LANES), all_axes)
    pair_gate = call(
        pair_gate_kernel, 8, pltpu.VMEM((pairs + channels, LANES), f32), 0, 5, devices=devices
    )(*map(far, (pair_flat, tri_in_gain[None], tri_gate, tri_out_gain[None], tri_out)))
    pair_next, updated, bias_tile = call(
        pair_out_kernel,
        8,
        (
            pltpu.HBM((pairs, channels), bf16),
            pltpu.HBM((pairs, channels), f32),
            whole((stripes, cols, rows, LANES), bf16),
        ),
        2,
        7,
        [pltpu.VMEM((devices * rows, LANES), f32)],
        width=width,
    )(
        here,
        chain_id,
        triangle,
        *map(
            far,
            (
                pair_flat,
                chain_id[None],
            ),
        ),
        near(pair_gate),
        *map(far, (bias_gain[None], bias_weight_t, chain_bias[None])),
    )
    head_bias = exchange(bias_tile.reshape(devices, rows, LANES), all_axes)
    share = length // cols
    part = pltpu.HBM((copies, share, hidden_width + 2 * LANES), bf16)
    bias_sums, outs, grads, *parts = call(
        attention_kernel,
        20,
        (
            pltpu.HBM((stripes, cols, rows, LANES), bf16),
            pltpu.HBM((tall, inner), bf16),
            pltpu.HBM((4, tall, inner), bf16),
            *[part] * cols,
        ),
        1,
        10,
        [
            pltpu.VMEM((local, length, length), f32),
            pltpu.VMEM((cols, copies, share, hidden_width + 2 * LANES), bf16),
        ],
        width=width,
        head_size=head_size,
    )(
        here,
        head_bias.reshape(stripes, cols, rows, LANES),
        *map(
            near,
            (query, key_rows, value, gated, gate_sig, grad_gated, scores, probs),
        ),
        far(weight_t),
    )
    bias_back = exchange(bias_sums.reshape(devices, rows, LANES), all_axes)
    received = [parts[0]] + [shift(parts[k], k) for k in range(1, cols)]
    others = []
    for k in range(1, cols):
        others.append(
            lax.ppermute(halves[k - 1], stripe_axes, [(i, i ^ 1) for i in range(stripes)])
        )
    chips = stripes // 2
    block = hidden_width // stripes
    keep, give = call(
        weight_in_kernel,
        16,
        (pltpu.VMEM((chips, block, 8 * LANES), bf16),) * 2,
        1,
        4,
        [pltpu.VMEM((chips, 2, block, 8 * LANES), bf16)],
    )(here, *map(far, (hidden_t, cot_t, grads, outs)))
    got = lax.ppermute(give, stripe_axes, [(i, i ^ 1) for i in range(stripes)])
    mine, *give = call(
        weight_add_kernel,
        12,
        (
            pltpu.HBM((block, 8 * LANES), bf16),
            *[pltpu.VMEM((block, 8 * LANES), bf16)] * (chips - 1),
        ),
        1,
        2,
        [pltpu.VMEM((chips, block, 8 * LANES), bf16)],
    )(here, near(keep), near(got))
    wires = [mine]
    for k in range(1, chips):
        wires.append(
            lax.ppermute(
                give[k - 1], stripe_axes, [(i, i ^ (2 * k)) for i in range(stripes)]
            )
        )
    pair_grad, weight_part = call(
        pair_back_kernel,
        8,
        (whole((pairs, channels), f32), whole((devices, heads_all, channels), bf16)),
        0,
        4,
        width=width,
    )(
        bias_back.reshape(stripes, cols, rows, LANES),
        *map(far, (updated, bias_gain[None], bias_weight_t)),
    )
    weight_part = exchange(weight_part, all_axes)
    bias_weight_grad = jnp.sum(weight_part.astype(f32), 0).T
    weight_grad, out_grad = call(
        weight_out_kernel,
        16,
        (
            whole((4, hidden_width // stripes, inner), f32),
            whole((inner, hidden_width // stripes), f32),
        ),
        0,
        chips,
    )(near(wires[0]), *map(near, wires[1:]))
    mine = pl.BlockSpec((copies, share, hidden_width), lambda i, here: (0, here[1], 0))
    fixed = lambda shape: pl.BlockSpec(shape, lambda i, here: (0,) * len(shape))
    denoised, token_grad = pl.pallas_call(
        token_out_kernel,
        grid_spec=pltpu.PrefetchScalarGridSpec(
            num_scalar_prefetch=1,
            grid=(1,),
            in_specs=[smem, mine, mine, fixed((1, hidden_width)), fixed((inner, hidden_width))]
            + [fixed((copies, share, hidden_width + 2 * LANES))] * cols
            + [fixed((inner // 2, hidden_width))] * (2 * cols - 2),
            out_specs=[fixed((copies, share, hidden_width))] * 2,
            scratch_shapes=[
                pltpu.VMEM((cols - 1, 2, inner // 2, hidden_width), bf16),
                pltpu.VMEM((copies * share, hidden_width), f32),
            ],
        ),
        out_shape=(whole((copies, share, hidden_width), bf16),) * 2,
        compiler_params=pltpu.CompilerParams(vmem_limit_bytes=16 << 20),
        name="token_out",
    )(
        here,
        scales,
        tokens,
        cotangent,
        attn_gain[None],
        out_weight,
        *received,
        *halves,
        *others,
    )
    return (
        pair_next.reshape(rows, width, channels),
        pair_grad.reshape(rows, width, channels),
        bias_weight_grad,
        denoised,
        token_grad,
        weight_grad,
        out_grad,
    )


def solution(mesh):
    return jax.shard_map(
        shards,
        mesh=mesh,
        in_specs=(
            P(("group", "row"), "col", None),
            P(("group", "row"), "col"),
            P(),
            P(),
            P(),
            P(),
            P(),
            P(),
            P(),
            P(),
            P(),
            P(("group", "row"), None, None),
            P(("group", "row")),
            P(),
            P(None, None, "col"),
            P("col", None),
            P(("group", "row"), None, None),
        ),
        out_specs=(
            P(("group", "row"), "col", None),
            P(("group", "row"), "col", None),
            P(),
            P(("group", "row"), "col", None),
            P(("group", "row"), "col", None),
            P(None, ("group", "row"), "col"),
            P("col", ("group", "row")),
        ),
        check_vma=False,
    )
```
